32 devices in a mesh: rep: 2 (over y), ep: 8 (over z, x), tp: 2 (over core).
Axes of the slice: x: 2, y: 2, z: 4, core: 2. Of those that a mesh axis runs over, the one named last changes fastest.
Arguments:
- tokens: bfloat16 [2048, 3584], P(('rep', 'ep'), 'tp'), parts along dimension 0, may hold values from -6 to 6
- expert_ids: int32 [2048, 8], P(('rep', 'ep')), parts along dimension 0, may hold values from 0 to 63, all different within a row; in each aligned block of 512 rows (0 to 511, 512 to 1023, ...) at most 128 rows name the same one
- gate_values: float32 [2048, 8], P(('rep', 'ep')), parts along dimension 0, may hold values from 0.1 to 1
- group_counts: int32 [4], P('rep'), parts along dimension 0, may hold values from 256 to 512
- gate_weight: bfloat16 [14336, 2560], P(('rep', 'ep'), 'tp'), parts along dimension 0, may hold values from -0.09375 to 0.09375
- up_weight: bfloat16 [14336, 2560], P(('rep', 'ep'), 'tp'), parts along dimension 0, may hold values from -0.09375 to 0.09375
- down_weight: bfloat16 [14336, 2560], P(('rep', 'ep'), 'tp'), parts along dimension 0, may hold values from -0.125 to 0.125
Outputs:
- expert_output: bfloat16 [2048, 3584], P(('rep', 'ep'), 'tp'), parts along dimension 0
The draws below stay inside these ranges and needn't reach their ends.
There are 2 independent parts, one for each index of `rep`. The reference program is written for one: setup_inputs(seed, part) draws one part's arguments, and reference() takes and returns one part's arrays. A program takes and returns all parts, laid end to end along the dimension named above; each array names one. Nothing has to cross between parts.
Inputs may be any that keep to these rules, and one draw needn't show every extreme that they name: `expert_ids`: each row names 8 different experts; within the 512 rows of one rollout group no expert is named by more than 128 rows.
All inputs are finite; a program needn't handle non-finite values.
Results may differ from the reference program's by a relative error of at most 0.014.
Values may be sent and summed in bfloat16 or wider, within the bound.
No kernel may reach another device: no remote copies, remote signals or barrier semaphores. Data moves between devices by JAX's collectives and lax.ppermute only.
A program may use at most 128 MiB of HBM per device.

```python
import math
import jax
import jax.numpy as jnp
import numpy as np
from jax import lax

D = 3584
FF = 2560
EXPERTS = 64
TOPK = 8
WAVE = 2
MEMBERS = 8
TOK_G = 512
CAP = 128
GROUPS = 2
TOKENS = 1024


def block_scale(rng, dims, split, least, top_value):
    loudness = 1.0
    for axis_at, parts in split:
        heights = jax.random.uniform(jax.random.fold_in(jax.random.fold_in(rng, 6), axis_at), (parts,), jnp.float32, least / len(split), top_value / len(split))
        loudness = loudness * jnp.repeat(jnp.exp(heights), dims[axis_at] // parts).reshape((-1,) + (1,) * (len(dims) - 1 - axis_at))
    return loudness


def routed_block(own_key, own, number, rows, count, top, most, slope):
    sequence = jax.random.permutation(own_key, count)
    crowded, common = shares(count, rows * top, most, slope, True), shares(count, rows * top, most, slope, False)
    places = jnp.arange(count)

    def named(tallies, rotation):
        used = int((tallies > 0).sum())
        fixed = max(1, used // 4)
        moved = fixed + (places - fixed + rotation * (used - fixed)) % max(1, count - fixed)
        return jnp.zeros((count,), jnp.int32).at[sequence[jnp.where(places < fixed, places, moved)]].set(jnp.asarray(tallies, jnp.int32))

    tallies = jnp.where(number % 4 == 0, named(crowded, number // 4), named(common, number - number // 4 - 1))
    mixed = jax.random.permutation(jax.random.fold_in(own, 3), count)
    source_of, taker = mixed[0:count // 2 * 2:2], mixed[1:count // 2 * 2:2]
    room = jnp.minimum(tallies[source_of] - 1, most - tallies[taker]) // 2
    room = jnp.where((source_of == sequence[0]) | (taker == sequence[0]) | (tallies[taker] == 0), 0, jnp.maximum(room, 0))
    moved = jax.random.randint(jax.random.fold_in(own, 4), (count // 2,), 0, 1 << 20) % (room + 1)
    tallies = tallies.at[source_of].add(-moved).at[taker].add(moved)
    members = jnp.searchsorted(jnp.cumsum(tallies), jnp.arange(rows * top), side="right").astype(jnp.int32)
    grid = members.reshape(top, rows).T
    grid = grid[jax.random.permutation(jax.random.fold_in(own, 1), rows)]
    rotation = jax.random.randint(jax.random.fold_in(own, 2), (rows, 1), 0, top)
    return jnp.take_along_axis(grid, (jnp.arange(top)[None, :] + rotation) % top, axis=1)


def shares(count, total, bound, lean, full):
    weights = [(1 << 20) // math.isqrt(grade ** lean) + 1 for grade in range(1, count + 1)]
    largest = bound if full else min(bound, max(-(-total // count), total * weights[0] // sum(weights)))
    least = 1 if total - largest >= count - 1 else 0
    holding, rest = [largest] + [least] * (count - 1), total - largest - least * (count - 1)
    while rest > 0:
        free = [i for i in range(1, count) if holding[i] < largest] or [i for i in range(1, count) if holding[i] < bound]
        pool, left = sum([weights[i] for i in free]), rest
        for i in free:
            extra = min(bound - holding[i], max(1, left * weights[i] // pool), rest)
            holding[i] = holding[i] + extra
            rest = rest - extra
    return np.array(holding)


def scatter_about(stream_key, dims, width, bound, shards=(), kind=jnp.bfloat16):
    values = width * jax.random.normal(stream_key, dims, jnp.float32)
    if shards:
        values = values * block_scale(stream_key, dims, shards, -0.22, 0.18)
    return jnp.clip(values, -bound, bound).astype(kind)


def setup_inputs(seed: int = 0, part: int = 0) -> dict:
    splits = jax.random.split(jax.random.key(seed), 8)
    own_keys = jax.random.split(jax.random.fold_in(splits[7], part), 8)
    tokens = scatter_about(own_keys[0], (TOKENS, D), 1.0, 6.0, ((0, 8), (1, 2)))
    expert_ids_keys = jax.random.split(jax.random.fold_in(own_keys[1], 1), TOKENS // TOK_G)
    expert_ids_turns = jax.random.permutation(jax.random.fold_in(own_keys[1], 3), TOKENS // TOK_G)
    expert_ids = jax.vmap(lambda own, number: routed_block(jax.random.fold_in(own_keys[1], 2), own, number, TOK_G, EXPERTS, TOPK, CAP, 2))(expert_ids_keys, expert_ids_turns).reshape((TOKENS, TOPK))
    gate_values = jnp.clip(0.1 + 0.9 * jax.random.uniform(own_keys[2], (TOKENS, TOPK), jnp.float32) ** block_scale(own_keys[2], (TOKENS, TOPK), ((0, 8),), -0.2, 0.2), 0.1, 1.0)
    group_counts = jax.random.randint(own_keys[3], (GROUPS,), TOK_G // 2, TOK_G + 1).astype(jnp.int32)
    gate_weight = scatter_about(own_keys[4], (WAVE * D, FF), D ** -0.5, 0.09375, ((0, 8), (1, 2)))
    up_weight = scatter_about(own_keys[5], (WAVE * D, FF), D ** -0.5, 0.09375, ((0, 8), (1, 2)))
    down_weight = scatter_about(own_keys[6], (WAVE * D, FF), FF ** -0.5, 0.125, ((0, 8), (1, 2)))
    return dict(tokens=tokens, expert_ids=expert_ids, gate_values=gate_values, group_counts=group_counts, gate_weight=gate_weight, up_weight=up_weight, down_weight=down_weight)


def dispatch_slots(expert_ids, gate_values, live_count, expert):
    row_index = jnp.arange(TOK_G, dtype=jnp.int32)
    live_rows = row_index < live_count
    hit_mask = expert_ids == expert
    selected = jnp.logical_and(jnp.any(hit_mask, axis=1), live_rows)
    row_weight = jnp.sum(jnp.where(hit_mask, gate_values, jnp.float32(0.0)), axis=1)
    position = jnp.cumsum(selected.astype(jnp.int32)) - 1
    slot_index = jnp.arange(CAP, dtype=jnp.int32)
    slot_match = jnp.logical_and(position[None, :] == slot_index[:, None], selected[None, :])
    slot_rows = jnp.sum(jnp.where(slot_match, row_index[None, :], 0), axis=1).astype(jnp.int32)
    slot_valid = jnp.any(slot_match, axis=1)
    slot_weight = jnp.where(slot_valid, row_weight[slot_rows], jnp.float32(0.0))
    return slot_rows, slot_weight


def one_group(group_tokens, expert_ids, gate_values, live_count, gate_weight, up_weight, down_weight):
    slice_width = FF // MEMBERS
    partials = jnp.zeros((MEMBERS, TOK_G, D), jnp.float32)
    for expert in range(WAVE):
        slot_rows, slot_weight = dispatch_slots(expert_ids, gate_values, live_count, expert)
        expert_rows = group_tokens[slot_rows]
        gate_act = jnp.dot(expert_rows, gate_weight[expert], preferred_element_type=jnp.float32)
        up_act = jnp.dot(expert_rows, up_weight[expert], preferred_element_type=jnp.float32)
        hidden = (jax.nn.silu(gate_act) * up_act).astype(jnp.bfloat16)
        for member in range(MEMBERS):
            hidden_piece = hidden[:, member * slice_width:(member + 1) * slice_width]
            down_piece = down_weight[expert][:, member * slice_width:(member + 1) * slice_width]
            projected = lax.dot_general(hidden_piece, down_piece, (((1,), (1,)), ((), ())), preferred_element_type=jnp.float32)
            partials = partials.at[member, slot_rows].add(slot_weight[:, None] * projected)
    rounded = lax.optimization_barrier(partials.astype(jnp.bfloat16)).astype(jnp.float32)
    return jnp.sum(rounded, axis=0).astype(jnp.bfloat16)


def reference(tokens, expert_ids, gate_values, group_counts, gate_weight, up_weight, down_weight):
    gate_blocks = gate_weight.reshape(WAVE, D, FF)
    up_blocks = up_weight.reshape(WAVE, D, FF)
    down_blocks = down_weight.reshape(WAVE, D, FF)

    def per_group(packed):
        group_tokens, group_ids, group_gates, live_count = packed
        return one_group(group_tokens, group_ids, group_gates, live_count, gate_blocks, up_blocks, down_blocks)

    combined = lax.map(per_group, (tokens.reshape(GROUPS, TOK_G, D), expert_ids.reshape(GROUPS, TOK_G, TOPK), gate_values.reshape(GROUPS, TOK_G, TOPK), group_counts))
    return combined.reshape(TOKENS, D)
```

```python
import functools

import jax
import jax.numpy as jnp
from jax import lax
from jax.experimental import pallas as pl
from jax.experimental.pallas import tpu as pltpu
from jax.sharding import PartitionSpec as P

D = 3584
FF = 2560
WAVE = 2
MEMBERS = 8
GROUP_EP = 4
TOK_G = 512
CAP = 128
LANES = 128
EXTRA = 16


def as_sent(array):

    def short(part):
        return part.astype(jnp.bfloat16) if part.dtype == jnp.float32 else part

    return jax.tree.map(short, array)


def swapped(array, axis, distance):
    return lax.ppermute(array, axis, [(i, i ^ 1 << distance) for i in range(lax.axis_size(axis))])


def dispatch_slots(expert_ids, gate_values, live_count, expert):
    row_index = jnp.arange(TOK_G, dtype=jnp.int32)
    live_rows = row_index < live_count
    hit_mask = expert_ids == expert
    selected = jnp.logical_and(jnp.any(hit_mask, axis=1), live_rows)
    row_weight = jnp.sum(jnp.where(hit_mask, gate_values, jnp.float32(0.0)), axis=1)
    position = jnp.cumsum(selected.astype(jnp.int32)) - 1
    slot_index = jnp.arange(CAP, dtype=jnp.int32)
    slot_match = jnp.logical_and(position[None, :] == slot_index[:, None], selected[None, :])
    slot_rows = jnp.sum(jnp.where(slot_match, row_index[None, :], 0), axis=1)
    slot_valid = jnp.any(slot_match, axis=1)
    slot_weight = jnp.where(slot_valid, row_weight[slot_rows], jnp.float32(0.0))
    return (slot_rows, slot_weight)


def travelling(tokens, expert_ids, gate_values, group_counts, gate_weight, up_weight, down_weight):
    ep_index = lax.axis_index("ep")
    slice_width = FF // MEMBERS
    group_bits = GROUP_EP.bit_length() - 1
    weight_stack = jnp.stack([gate_weight, up_weight, down_weight])
    rows_held = weight_stack.shape[1]
    pieces = weight_stack.shape[2] // slice_width
    slice_blocks = weight_stack.reshape(3, rows_held, pieces, slice_width).transpose(0, 2, 1, 3)
    fan_out = lax.axis_size("ep") // pieces
    outgoing = jnp.tile(slice_blocks, (1, fan_out, 1, 1))
    arrived = lax.all_to_all(outgoing, "ep", split_axis=1, concat_axis=1, tiled=True)
    columns = arrived.reshape(3, -1, slice_width)
    features = lax.all_gather(tokens, "tp", axis=1, tiled=True)
    group_data = (features, expert_ids, gate_values)
    for bit_level in range(group_bits):
        received = jax.tree.map(
            lambda part, own: part.astype(own.dtype),
            swapped(as_sent(group_data), "ep", bit_level),
            group_data,
        )
        upper_half = ep_index >> bit_level & 1 == 1
        group_data = tuple(
            (
                jnp.where(
                    upper_half, jnp.concatenate([other, own], 0), jnp.concatenate([own, other], 0)
                )
                for own, other in zip(group_data, received)
            )
        )
    group_tokens, group_ids, group_gates = group_data
    live_count = lax.dynamic_index_in_dim(group_counts, ep_index // GROUP_EP, keepdims=False)
    partials = jnp.zeros((group_tokens.shape[0], D), jnp.float32)
    for expert in range(WAVE):
        slot_rows, slot_weight = dispatch_slots(group_ids, group_gates, live_count, expert)
        expert_rows = group_tokens[slot_rows]
        gate_cols = columns[0, expert * D : (expert + 1) * D]
        up_cols = columns[1, expert * D : (expert + 1) * D]
        down_cols = columns[2, expert * D : (expert + 1) * D]
        gate_act = jnp.dot(expert_rows, gate_cols, preferred_element_type=jnp.float32)
        up_act = jnp.dot(expert_rows, up_cols, preferred_element_type=jnp.float32)
        hidden = (jax.nn.silu(gate_act) * up_act).astype(jnp.bfloat16)
        projected = lax.dot_general(
            hidden, down_cols, (((1,), (1,)), ((), ())), preferred_element_type=jnp.float32
        )
        partials = partials.at[slot_rows].add(slot_weight[:, None] * projected)
    rounded = lax.optimization_barrier(partials.astype(jnp.bfloat16)).astype(jnp.float32)
    halved = lax.psum_scatter(
        rounded.astype(jnp.bfloat16), "tp", scatter_dimension=1, tiled=True
    ).astype(jnp.float32)
    for bit_level in reversed(range(group_bits)):
        paired_up = halved.reshape(2, -1, halved.shape[1])
        upper_half = ep_index >> bit_level & 1 == 1
        kept_part = jnp.where(upper_half, paired_up[1], paired_up[0])
        sent_part = jnp.where(upper_half, paired_up[0], paired_up[1])
        halved = kept_part + swapped(sent_part.astype(jnp.bfloat16), "ep", bit_level).astype(
            sent_part.dtype
        )
    return halved.astype(jnp.bfloat16)


def pack_kernel(info, tokens, expert_ids, gate_values, even_ref, odd_ref):
    parity, live, own = info[0], info[1], info[2]
    rows = tokens.shape[0]
    width = even_ref.shape[1]
    for block, ref in ((parity, even_ref), (1 - parity, odd_ref)):
        ref[:rows, :] = tokens[:, pl.ds(pl.multiple_of(block * width, LANES), width)]
    is_live = lax.broadcasted_iota(jnp.int32, (rows, 1), 0) < live
    ids = expert_ids[...]
    lane = lax.broadcasted_iota(jnp.int32, (rows, LANES), 1)
    table = jnp.zeros((rows, LANES), jnp.float32)
    for place, expert in enumerate((own, WAVE - 1 - own)):
        named = jnp.where(ids == expert, gate_values[...], 0.0)
        weight = jnp.where(is_live, jnp.sum(named, axis=1, keepdims=True), 0.0)
        table = jnp.where(lane == place, weight, table)
    rest = table.T[:EXTRA, :]
    for ref in (even_ref, odd_ref):
        ref[rows:, :] = jnp.zeros((EXTRA, width), ref.dtype)
    for term in range(3):
        part = rest.astype(jnp.bfloat16)
        rest = rest - part.astype(jnp.float32)
        for ref in (even_ref, odd_ref):
            ref[rows:, term * LANES : (term + 1) * LANES] = part


def routing_of(block, rows):
    extra = block[rows:, : 3 * LANES].astype(jnp.float32)
    return extra[:, :LANES] + extra[:, LANES : 2 * LANES] + extra[:, 2 * LANES :]


def compact_kernel(info, *refs):
    blocks, (own_ref, other_ref, place_ref, weight_ref) = refs[:-4], refs[-4:]
    member = info[1]
    slots = own_ref.shape[0]
    rows = blocks[0].shape[0] - EXTRA
    before = lax.broadcasted_iota(jnp.int32, (rows, rows), 0)
    after = lax.broadcasted_iota(jnp.int32, (rows, rows), 1)
    upto = (before <= after).astype(jnp.float32).astype(jnp.bfloat16)
    slot = lax.broadcasted_iota(jnp.int32, (slots, rows), 0)
    total = jnp.zeros((2 * slots, own_ref.shape[1]), jnp.float32)
    weights = [routing_of(block, rows) for block in blocks]
    counts = [
        jnp.dot(
            (weight > 0.0).astype(jnp.float32).astype(jnp.bfloat16),
            upto,
            preferred_element_type=jnp.float32,
        )
        for weight in weights
    ]
    for turn, block in enumerate(blocks):
        weight, count = weights[turn], counts[turn]
        for before, earlier in enumerate(counts):
            if before != turn:
                ahead = jnp.bitwise_xor(member, before) < jnp.bitwise_xor(member, turn)
                count = count + jnp.where(ahead, earlier[:, rows - 1 :], 0.0)
        place = jnp.where(weight > 0.0, count - 1.0, -1.0).astype(jnp.int32)
        pick = jnp.concatenate(
            [(slot == place[e : e + 1, :]).astype(jnp.float32) for e in range(WAVE)], 0
        ).astype(jnp.bfloat16)
        total = total + jnp.dot(pick, block[:rows, :], preferred_element_type=jnp.float32)
        place_ref[turn] = place[:8]
        weight_ref[turn] = weight[:8]
    own_ref[...] = total[:slots].astype(own_ref.dtype)
    other_ref[...] = total[slots:].astype(other_ref.dtype)


def spread_kernel(place_ref, weight_ref, pick_ref, column_ref):
    rows = place_ref.shape[2]
    slot = lax.broadcasted_iota(jnp.int32, (CAP, rows), 0)
    for turn in range(place_ref.shape[0]):
        place, weight = place_ref[turn], weight_ref[turn]
        for e in range(WAVE):
            pick = (slot == place[e : e + 1, :]).astype(jnp.float32)
            pick_ref[turn, :, e * CAP : (e + 1) * CAP] = pick.T.astype(pick_ref.dtype)
        table = jnp.where(slot == 0, weight[0:1, :], jnp.where(slot == 1, weight[1:2, :], 0.0))
        column_ref[turn] = table.T


def gate_up_kernel(members, info, own_ref, other_ref, *refs):
    held, came = refs[0:2], refs[2:4]
    outs, (buffer, sem) = refs[4 : 4 + members], refs[4 + members :]
    use_own, member, core = info[0], info[1], info[2]
    width = buffer.shape[3]
    per_half = held[0].shape[1] // width
    order = [members - 1 - n for n in range(members)]

    def copies(source, turn, column):
        return [
            pltpu.make_async_copy(
                source[n].at[:, pl.ds(pl.multiple_of(column * width, LANES), width)],
                buffer.at[turn, n],
                sem.at[turn, n],
            )
            for n in range(2)
        ]

    for turn in order:
        block = jnp.bitwise_xor(member, turn)
        half, column = block // per_half, block % per_half

        @pl.when(half == core)
        def _():
            for copy in copies(held, turn, column):
                copy.start()

        @pl.when(half != core)
        def _():
            for copy in copies(came, turn, column):
                copy.start()

    rows = jnp.where(use_own == 1, own_ref[...], other_ref[...])
    for turn in order:
        for n, copy in enumerate(copies(held, turn, 0)):
            copy.wait()
            outs[turn][:, n * width : (n + 1) * width] = jnp.dot(
                rows, buffer[turn, n], preferred_element_type=jnp.float32
            ).astype(outs[turn].dtype)


def down_kernel(members, info, *refs):
    hidden, held, came = refs[:members], refs[members], refs[members + 1]
    out_ref, buffer, sem = refs[members + 2 :]
    member, core = info[1], info[2]
    width = buffer.shape[2]
    per_half = held.shape[1] // width

    def copy_of(source, turn, column):
        return pltpu.make_async_copy(
            source.at[:, pl.ds(pl.multiple_of(column * width, LANES), width)],
            buffer.at[turn],
            sem.at[turn],
        )

    for turn in range(members):
        block = jnp.bitwise_xor(member, turn)
        half, column = block // per_half, block % per_half

        @pl.when(half == core)
        def _():
            copy_of(held, turn, column).start()

        @pl.when(half != core)
        def _():
            copy_of(came, turn, column).start()

    total = None
    for turn in range(members):
        copy_of(held, turn, 0).wait()
        product = lax.dot_general(
            hidden[turn][...],
            buffer[turn],
            (((1,), (1,)), ((), ())),
            preferred_element_type=jnp.float32,
        )
        total = product if total is None else total + product
    out_ref[...] = total.astype(out_ref.dtype)


def expand_kernel(own_ref, other_ref, pick_ref, column_ref, *outs):
    for turn, out in enumerate(outs):
        total = None
        for e, ref in enumerate((own_ref, other_ref)):
            chosen = jnp.dot(
                pick_ref[turn, :, e * CAP : (e + 1) * CAP],
                ref[...],
                preferred_element_type=jnp.float32,
            )
            part = column_ref[turn, :, e : e + 1] * chosen
            total = part if total is None else total + part
        out[...] = total.astype(out.dtype)


VMEM = pl.BlockSpec(memory_space=pltpu.VMEM)
SMEM = pl.BlockSpec(memory_space=pltpu.SMEM)
ANY = pl.BlockSpec(memory_space=pl.ANY)


def call(kernel, name, outs, specs, scratch=(), mib=8):
    return pl.pallas_call(
        kernel,
        out_shape=[jax.ShapeDtypeStruct(shape, dtype) for shape, dtype in outs],
        in_specs=specs,
        out_specs=[VMEM] * len(outs),
        scratch_shapes=list(scratch),
        compiler_params=pltpu.CompilerParams(vmem_limit_bytes=mib * 1024 * 1024),
        name=name,
    )


def moved(array, ep_size, tp_size, target):
    pairs = []
    for ep in range(ep_size):
        for tp in range(tp_size):
            to = target(ep, tp)
            if to is not None:
                pairs.append((ep * tp_size + tp, to[0] * tp_size + to[1]))
    return lax.ppermute(array, ("ep", "tp"), pairs)


def resting(
    tokens, expert_ids, gate_values, group_counts, gate_weight, up_weight, down_weight
):
    ep_size, tp_size = lax.axis_size("ep"), lax.axis_size("tp")
    ep, core = lax.axis_index("ep"), lax.axis_index("tp")
    rows = tokens.shape[0]
    members = TOK_G // rows
    per_core = members // tp_size
    square, member = ep // members, ep % members
    thick = gate_weight.shape[0]
    width = tp_size * gate_weight.shape[1] // members
    bf16, f32 = jnp.bfloat16, jnp.float32
    send = functools.partial(moved, ep_size=ep_size, tp_size=tp_size)

    live = lax.dynamic_index_in_dim(group_counts, square, keepdims=False) - member * rows
    pack_info = jnp.stack([member % per_core, live, square]).astype(jnp.int32)
    packed = call(pack_kernel, "pack", [((rows + EXTRA, thick), bf16)] * 2, [SMEM] + [VMEM] * 3)(
        pack_info, tokens, expert_ids, gate_values
    )

    def home(turn):
        def target(e, t):
            to = e % members ^ turn
            return (e // members * members + to, e // members) if to // per_core == t else None

        return target

    arrived = [
        send(packed[turn % per_core], target=home(turn)) for turn in range(members)
    ]
    other_half = [(t, tp_size - 1 - t) for t in range(tp_size)]
    gate_came, up_came, down_came = (
        lax.ppermute(weight, "tp", other_half) for weight in (gate_weight, up_weight, down_weight)
    )

    info = jnp.stack([(core == square).astype(jnp.int32), member, core]).astype(jnp.int32)
    own_rows, other_rows, place, weight = call(
        compact_kernel,
        "compact",
        [
            ((CAP, thick), bf16),
            ((CAP, thick), bf16),
            ((members, 8, rows), jnp.int32),
            ((members, 8, rows), f32),
        ],
        [SMEM] + [VMEM] * members,
    )(info, *arrived)
    across = lambda from_own: lambda e, t: (
        ((e + members) % ep_size, t) if (t == e // members) == from_own else None
    )
    came_rows = send(other_rows, target=across(True))
    pick, column = call(
        spread_kernel,
        "spread",
        [((members, rows, WAVE * CAP), bf16), ((members, rows, LANES), f32)],
        [VMEM] * 2,
    )(place, weight)

    sums = call(
        functools.partial(gate_up_kernel, members),
        "gate_up",
        [((CAP, 2 * width), f32)] + [((CAP, 2 * width), bf16)] * (members - 1),
        [SMEM, VMEM, VMEM] + [ANY] * 4,
        [
            pltpu.VMEM((members, 2, thick, width), bf16),
            pltpu.SemaphoreType.DMA((members, 2)),
        ],
        16,
    )(info, own_rows, came_rows, gate_weight, up_weight, gate_came, up_came)
    partner = lambda turn: lambda e, t: (e ^ turn, t)
    order = [members - 1 - n for n in range(members - 1)]
    came_sums = [send(sums[turn], target=partner(turn)) for turn in order]
    whole = sums[0] + sum(part.astype(f32) for part in came_sums)
    gate, up = whole[:, :width], whole[:, width:]
    hidden = (jax.nn.silu(gate) * up).astype(bf16)

    came_hidden = {turn: send(hidden, target=partner(turn)) for turn in order}
    all_hidden = [hidden] + [came_hidden[turn] for turn in range(1, members)]
    (projected,) = call(
        functools.partial(down_kernel, members),
        "down",
        [((CAP, thick), bf16)],
        [SMEM] + [VMEM] * members + [ANY] * 2,
        [pltpu.VMEM((members, thick, width), bf16), pltpu.SemaphoreType.DMA((members,))],
        16,
    )(info, *all_hidden, down_weight, down_came)
    came_projected = send(projected, target=across(False))

    spread = call(
        expand_kernel, "expand", [((rows, thick), bf16)] * members, [VMEM] * 4
    )(projected, came_projected, pick, column)

    def back(turn):
        def target(e, t):
            if e // members != t:
                return None
            return (e ^ turn, e % members // per_core)

        return target

    returned = [send(spread[turn], target=back(turn)) for turn in range(members)]
    even = sum(returned[turn].astype(f32) for turn in range(0, members, 2))
    odd = sum(returned[turn].astype(f32) for turn in range(1, members, 2))
    swap = member % per_core == 1
    return jnp.concatenate(
        [jnp.where(swap, odd, even), jnp.where(swap, even, odd)], axis=1
    ).astype(bf16)


def shards(tokens, expert_ids, gate_values, group_counts, gate_weight, up_weight, down_weight):
    ep_size, tp_size = lax.axis_size("ep"), lax.axis_size("tp")
    members = TOK_G // tokens.shape[0]
    rests = ep_size == WAVE * members and tp_size == WAVE and members == 2 * tp_size
    return (resting if rests else travelling)(
        tokens, expert_ids, gate_values, group_counts, gate_weight, up_weight, down_weight
    )


def solution(mesh):
    placed = (
        P(("rep", "ep"), "tp"),
        P(("rep", "ep"), None),
        P(("rep", "ep"), None),
        P("rep"),
        P(("rep", "ep"), "tp"),
        P(("rep", "ep"), "tp"),
        P(("rep", "ep"), "tp"),
    )
    return jax.shard_map(
        shards, mesh=mesh, in_specs=placed, out_specs=P(("rep", "ep"), "tp"), check_vma=False
    )
```

```python
import functools

import jax
import jax.numpy as jnp
from jax import lax
from jax.experimental import pallas as pl
from jax.experimental.pallas import tpu as pltpu
from jax.sharding import PartitionSpec as P

D = 3584
FF = 2560
WAVE = 2
MEMBERS = 8
GROUP_EP = 4
TOK_G = 512
CAP = 128
LANES = 128
EXTRA = 16


def as_sent(array):

    def short(part):
        return part.astype(jnp.bfloat16) if part.dtype == jnp.float32 else part

    return jax.tree.map(short, array)


def swapped(array, axis, distance):
    return lax.ppermute(array, axis, [(i, i ^ 1 << distance) for i in range(lax.axis_size(axis))])


def dispatch_slots(expert_ids, gate_values, live_count, expert):
    row_index = jnp.arange(TOK_G, dtype=jnp.int32)
    live_rows = row_index < live_count
    hit_mask = expert_ids == expert
    selected = jnp.logical_and(jnp.any(hit_mask, axis=1), live_rows)
    row_weight = jnp.sum(jnp.where(hit_mask, gate_values, jnp.float32(0.0)), axis=1)
    position = jnp.cumsum(selected.astype(jnp.int32)) - 1
    slot_index = jnp.arange(CAP, dtype=jnp.int32)
    slot_match = jnp.logical_and(position[None, :] == slot_index[:, None], selected[None, :])
    slot_rows = jnp.sum(jnp.where(slot_match, row_index[None, :], 0), axis=1)
    slot_valid = jnp.any(slot_match, axis=1)
    slot_weight = jnp.where(slot_valid, row_weight[slot_rows], jnp.float32(0.0))
    return (slot_rows, slot_weight)


def travelling(tokens, expert_ids, gate_values, group_counts, gate_weight, up_weight, down_weight):
    ep_index = lax.axis_index("ep")
    slice_width = FF // MEMBERS
    group_bits = GROUP_EP.bit_length() - 1
    weight_stack = jnp.stack([gate_weight, up_weight, down_weight])
    rows_held = weight_stack.shape[1]
    pieces = weight_stack.shape[2] // slice_width
    slice_blocks = weight_stack.reshape(3, rows_held, pieces, slice_width).transpose(0, 2, 1, 3)
    fan_out = lax.axis_size("ep") // pieces
    outgoing = jnp.tile(slice_blocks, (1, fan_out, 1, 1))
    arrived = lax.all_to_all(outgoing, "ep", split_axis=1, concat_axis=1, tiled=True)
    columns = arrived.reshape(3, -1, slice_width)
    features = lax.all_gather(tokens, "tp", axis=1, tiled=True)
    group_data = (features, expert_ids, gate_values)
    for bit_level in range(group_bits):
        received = jax.tree.map(
            lambda part, own: part.astype(own.dtype),
            swapped(as_sent(group_data), "ep", bit_level),
            group_data,
        )
        upper_half = ep_index >> bit_level & 1 == 1
        group_data = tuple(
            (
                jnp.where(
                    upper_half, jnp.concatenate([other, own], 0), jnp.concatenate([own, other], 0)
                )
                for own, other in zip(group_data, received)
            )
        )
    group_tokens, group_ids, group_gates = group_data
    live_count = lax.dynamic_index_in_dim(group_counts, ep_index // GROUP_EP, keepdims=False)
    partials = jnp.zeros((group_tokens.shape[0], D), jnp.float32)
    for expert in range(WAVE):
        slot_rows, slot_weight = dispatch_slots(group_ids, group_gates, live_count, expert)
        expert_rows = group_tokens[slot_rows]
        gate_cols = columns[0, expert * D : (expert + 1) * D]
        up_cols = columns[1, expert * D : (expert + 1) * D]
        down_cols = columns[2, expert * D : (expert + 1) * D]
        gate_act = jnp.dot(expert_rows, gate_cols, preferred_element_type=jnp.float32)
        up_act = jnp.dot(expert_rows, up_cols, preferred_element_type=jnp.float32)
        hidden = (jax.nn.silu(gate_act) * up_act).astype(jnp.bfloat16)
        projected = lax.dot_general(
            hidden, down_cols, (((1,), (1,)), ((), ())), preferred_element_type=jnp.float32
        )
        partials = partials.at[slot_rows].add(slot_weight[:, None] * projected)
    rounded = lax.optimization_barrier(partials.astype(jnp.bfloat16)).astype(jnp.float32)
    halved = lax.psum_scatter(
        rounded.astype(jnp.bfloat16), "tp", scatter_dimension=1, tiled=True
    ).astype(jnp.float32)
    for bit_level in reversed(range(group_bits)):
        paired_up = halved.reshape(2, -1, halved.shape[1])
        upper_half = ep_index >> bit_level & 1 == 1
        kept_part = jnp.where(upper_half, paired_up[1], paired_up[0])
        sent_part = jnp.where(upper_half, paired_up[0], paired_up[1])
        halved = kept_part + swapped(sent_part.astype(jnp.bfloat16), "ep", bit_level).astype(
            sent_part.dtype
        )
    return halved.astype(jnp.bfloat16)


def place_of(members):
    ep = lax.axis_index("ep")
    return ep // members, ep % members, lax.axis_index("tp")


def pack_kernel(members, counts, tokens, expert_ids, gate_values, *refs):
    outs, (table_ref, sem) = refs[:2], refs[2:]
    square, member, core = place_of(members)
    rows = tokens.shape[0]
    width = outs[0].shape[1]
    parity = member % 2
    copies = [
        pltpu.make_async_copy(
            tokens.at[:, pl.ds(pl.multiple_of(block * width, LANES), width)],
            out.at[:rows],
            sem.at[n],
        )
        for n, (block, out) in enumerate(zip((parity, 1 - parity), outs))
    ]
    for copy in copies:
        copy.start()
    is_live = lax.broadcasted_iota(jnp.int32, (1, rows), 1) < counts[square] - member * rows
    ids, gates = expert_ids[...], gate_values[...]
    place = lax.broadcasted_iota(jnp.int32, (EXTRA, rows), 0)
    rest = jnp.zeros((EXTRA, rows), jnp.float32)
    for n, expert in enumerate((square, WAVE - 1 - square)):
        named = jnp.sum(jnp.where(ids == expert, gates, 0.0), axis=0, keepdims=True)
        rest = jnp.where(place == n, jnp.where(is_live, named, 0.0), rest)
    table_ref[...] = jnp.zeros(table_ref.shape, table_ref.dtype)
    for term in range(3):
        part = rest.astype(jnp.bfloat16)
        rest = rest - part.astype(jnp.float32)
        table_ref[:, term * rows : (term + 1) * rows] = part
    tables = [
        pltpu.make_async_copy(table_ref, out.at[rows:], sem.at[2 + n])
        for n, out in enumerate(outs)
    ]
    for copy in tables:
        copy.start()
    for copy in copies + tables:
        copy.wait()


def routing_of(block, rows):
    extra = block[rows:, : 3 * LANES].astype(jnp.float32)
    return extra[:, :LANES] + extra[:, LANES : 2 * LANES] + extra[:, 2 * LANES :]


def compact_kernel(*refs):
    blocks, (own_ref, other_ref, place_ref, weight_ref) = refs[:-4], refs[-4:]
    member = place_of(len(blocks))[1]
    slots = own_ref.shape[0]
    rows = blocks[0].shape[0] - EXTRA
    before = lax.broadcasted_iota(jnp.int32, (rows, rows), 0)
    after = lax.broadcasted_iota(jnp.int32, (rows, rows), 1)
    upto = (before <= after).astype(jnp.float32).astype(jnp.bfloat16)
    slot = lax.broadcasted_iota(jnp.int32, (slots, rows), 0)
    total = jnp.zeros((2 * slots, own_ref.shape[1]), jnp.float32)
    weights = [routing_of(block, rows) for block in blocks]
    counts = [
        jnp.dot(
            (weight > 0.0).astype(jnp.float32).astype(jnp.bfloat16),
            upto,
            preferred_element_type=jnp.float32,
        )
        for weight in weights
    ]
    for turn, block in enumerate(blocks):
        weight, count = weights[turn], counts[turn]
        for before, earlier in enumerate(counts):
            if before != turn:
                ahead = jnp.bitwise_xor(member, before) < jnp.bitwise_xor(member, turn)
                count = count + jnp.where(ahead, earlier[:, rows - 1 :], 0.0)
        place = jnp.where(weight > 0.0, count - 1.0, -1.0).astype(jnp.int32)
        pick = jnp.concatenate(
            [(slot == place[e : e + 1, :]).astype(jnp.float32) for e in range(WAVE)], 0
        ).astype(jnp.bfloat16)
        total = total + jnp.dot(pick, block[:rows, :], preferred_element_type=jnp.float32)
        place_ref[turn] = place[:8]
        weight_ref[turn] = weight[:8]
    own_ref[...] = total[:slots].astype(own_ref.dtype)
    other_ref[...] = total[slots:].astype(other_ref.dtype)


def spread_kernel(place_ref, weight_ref, pick_ref, column_ref):
    rows = place_ref.shape[2]
    slot = lax.broadcasted_iota(jnp.int32, (CAP, rows), 0)
    for turn in range(place_ref.shape[0]):
        place, weight = place_ref[turn], weight_ref[turn]
        for e in range(WAVE):
            pick = (slot == place[e : e + 1, :]).astype(jnp.float32)
            pick_ref[turn, :, e * CAP : (e + 1) * CAP] = pick.T.astype(pick_ref.dtype)
        table = jnp.where(slot == 0, weight[0:1, :], jnp.where(slot == 1, weight[1:2, :], 0.0))
        column_ref[turn] = table.T


def gate_up_kernel(members, own_ref, other_ref, *refs):
    held, came = refs[0:2], refs[2:4]
    outs, (buffer, sem) = refs[4 : 4 + members], refs[4 + members :]
    square, member, core = place_of(members)
    width = buffer.shape[3]
    per_half = held[0].shape[1] // width
    order = [members - 1 - n for n in range(members)]

    def copies(source, turn, column):
        return [
            pltpu.make_async_copy(
                source[n].at[:, pl.ds(pl.multiple_of(column * width, LANES), width)],
                buffer.at[turn, n],
                sem.at[turn, n],
            )
            for n in range(2)
        ]

    for turn in order:
        block = jnp.bitwise_xor(member, turn)
        half, column = block // per_half, block % per_half

        @pl.when(half == core)
        def _():
            for copy in copies(held, turn, column):
                copy.start()

        @pl.when(half != core)
        def _():
            for copy in copies(came, turn, column):
                copy.start()

    rows = jnp.where(square == core, own_ref[...], other_ref[...])
    for turn in order:
        for n, copy in enumerate(copies(held, turn, 0)):
            copy.wait()
            outs[turn][:, n * width : (n + 1) * width] = jnp.dot(
                rows, buffer[turn, n], preferred_element_type=jnp.float32
            ).astype(outs[turn].dtype)


def down_kernel(members, *refs):
    hidden, held, came = refs[:members], refs[members], refs[members + 1]
    out_ref, buffer, sem = refs[members + 2 :]
    member, core = place_of(members)[1:]
    width = buffer.shape[2]
    per_half = held.shape[1] // width

    def copy_of(source, turn, column):
        return pltpu.make_async_copy(
            source.at[:, pl.ds(pl.multiple_of(column * width, LANES), width)],
            buffer.at[turn],
            sem.at[turn],
        )

    for turn in range(members):
        block = jnp.bitwise_xor(member, turn)
        half, column = block // per_half, block % per_half

        @pl.when(half == core)
        def _():
            copy_of(held, turn, column).start()

        @pl.when(half != core)
        def _():
            copy_of(came, turn, column).start()

    total = None
    for turn in range(members):
        copy_of(held, turn, 0).wait()
        product = lax.dot_general(
            hidden[turn][...],
            buffer[turn],
            (((1,), (1,)), ((), ())),
            preferred_element_type=jnp.float32,
        )
        total = product if total is None else total + product
    out_ref[...] = total.astype(out_ref.dtype)


def expand_kernel(own_ref, other_ref, pick_ref, column_ref, *outs):
    for turn, out in enumerate(outs):
        total = None
        for e, ref in enumerate((own_ref, other_ref)):
            chosen = jnp.dot(
                pick_ref[turn, :, e * CAP : (e + 1) * CAP],
                ref[...],
                preferred_element_type=jnp.float32,
            )
            part = column_ref[turn, :, e : e + 1] * chosen
            total = part if total is None else total + part
        out[...] = total.astype(out.dtype)


VMEM = pl.BlockSpec(memory_space=pltpu.VMEM)
SMEM = pl.BlockSpec(memory_space=pltpu.SMEM)
HBM = pl.BlockSpec(memory_space=pltpu.HBM)


def call(kernel, name, outs, specs, scratch=(), mib=8, space=VMEM):
    return pl.pallas_call(
        kernel,
        out_shape=[jax.ShapeDtypeStruct(shape, dtype) for shape, dtype in outs],
        in_specs=specs,
        out_specs=[space] * len(outs),
        scratch_shapes=list(scratch),
        compiler_params=pltpu.CompilerParams(vmem_limit_bytes=mib * 1024 * 1024),
        name=name,
    )


def moved(array, ep_size, tp_size, target):
    targets = {(e, t): target(e, t) for e in range(ep_size) for t in range(tp_size)}
    used = set(targets.values())
    pairs = []
    for (e, t), to in targets.items():
        if to is None:
            (to,) = [(e, core) for core in range(tp_size) if (e, core) not in used]
        pairs.append((e * tp_size + t, to[0] * tp_size + to[1]))
    return lax.ppermute(array, ("ep", "tp"), pairs)


def resting(
    tokens, expert_ids, gate_values, group_counts, gate_weight, up_weight, down_weight
):
    ep_size, tp_size = lax.axis_size("ep"), lax.axis_size("tp")
    ep, core = lax.axis_index("ep"), lax.axis_index("tp")
    rows = tokens.shape[0]
    members = TOK_G // rows
    per_core = members // tp_size
    member = ep % members
    thick = gate_weight.shape[0]
    width = tp_size * gate_weight.shape[1] // members
    bf16, f32 = jnp.bfloat16, jnp.float32
    send = functools.partial(moved, ep_size=ep_size, tp_size=tp_size)
    bind = lambda kernel: functools.partial(kernel, members)
    turns = [members - 1 - n for n in range(members)]

    packed = call(
        bind(pack_kernel),
        "pack",
        [((rows + EXTRA, thick), bf16)] * 2,
        [SMEM, HBM, VMEM, VMEM],
        [pltpu.VMEM((EXTRA, thick), bf16), pltpu.SemaphoreType.DMA((4,))],
        space=HBM,
    )(group_counts, tokens, expert_ids.T, gate_values.T)

    def home(turn):
        def target(e, t):
            to = e % members ^ turn
            return (e // members * members + to, e // members) if to // per_core == t else None

        return target

    sent = {turn: send(packed[turn % 2], target=home(turn)) for turn in turns}
    arrived = [sent[turn] for turn in range(members)]
    other_half = [(t, tp_size - 1 - t) for t in range(tp_size)]
    gate_came, up_came, down_came = (
        lax.ppermute(weight, "tp", other_half) for weight in (gate_weight, up_weight, down_weight)
    )

    own_rows, other_rows, place, weight = call(
        compact_kernel,
        "compact",
        [
            ((CAP, thick), bf16),
            ((CAP, thick), bf16),
            ((members, 8, rows), jnp.int32),
            ((members, 8, rows), f32),
        ],
        [VMEM] * members,
    )(*arrived)
    across = lambda from_own: lambda e, t: (
        ((e + members) % ep_size, t) if (t == e // members) == from_own else None
    )
    came_rows = send(other_rows, target=across(True))
    pick, column = call(
        spread_kernel,
        "spread",
        [((members, rows, WAVE * CAP), bf16), ((members, rows, LANES), f32)],
        [VMEM] * 2,
    )(place, weight)

    sums = call(
        bind(gate_up_kernel),
        "gate_up",
        [((CAP, 2 * width), f32)] + [((CAP, 2 * width), bf16)] * (members - 1),
        [VMEM, VMEM] + [HBM] * 4,
        [
            pltpu.VMEM((members, 2, thick, width), bf16),
            pltpu.SemaphoreType.DMA((members, 2)),
        ],
        16,
    )(own_rows, came_rows, gate_weight, up_weight, gate_came, up_came)
    partner = lambda turn: lambda e, t: (e ^ turn, t)
    came_sums = [send(sums[turn], target=partner(turn)) for turn in turns[:-1]]
    whole = sums[0] + sum(part.astype(f32) for part in came_sums)
    gate, up = whole[:, :width], whole[:, width:]
    hidden = (jax.nn.silu(gate) * up).astype(bf16)

    came_hidden = {turn: send(hidden, target=partner(turn)) for turn in turns[:-1]}
    all_hidden = [hidden] + [came_hidden[turn] for turn in range(1, members)]
    (projected,) = call(
        bind(down_kernel),
        "down",
        [((CAP, thick), bf16)],
        [VMEM] * members + [HBM] * 2,
        [pltpu.VMEM((members, thick, width), bf16), pltpu.SemaphoreType.DMA((members,))],
        16,
    )(*all_hidden, down_weight, down_came)
    came_projected = send(projected, target=across(False))

    spread = call(
        expand_kernel, "expand", [((rows, thick), bf16)] * members, [VMEM] * 4
    )(projected, came_projected, pick, column)

    def back(turn):
        def target(e, t):
            return (e ^ turn, e % members // per_core) if e // members == t else None

        return target

    returned = {turn: send(spread[turn], target=back(turn)) for turn in turns}
    low = core == member // per_core
    even, odd = (jnp.where(low, returned[n], returned[n + per_core]) for n in range(per_core))
    swap = member % per_core == 1
    return jnp.concatenate([jnp.where(swap, odd, even), jnp.where(swap, even, odd)], axis=1)


def shards(tokens, expert_ids, gate_values, group_counts, gate_weight, up_weight, down_weight):
    ep_size, tp_size = lax.axis_size("ep"), lax.axis_size("tp")
    members = TOK_G // tokens.shape[0]
    rests = ep_size == WAVE * members and tp_size == WAVE and members == 2 * tp_size
    return (resting if rests else travelling)(
        tokens, expert_ids, gate_values, group_counts, gate_weight, up_weight, down_weight
    )


def solution(mesh):
    placed = (
        P(("rep", "ep"), "tp"),
        P(("rep", "ep"), None),
        P(("rep", "ep"), None),
        P("rep"),
        P(("rep", "ep"), "tp"),
        P(("rep", "ep"), "tp"),
        P(("rep", "ep"), "tp"),
    )
    return jax.shard_map(
        shards, mesh=mesh, in_specs=placed, out_specs=P(("rep", "ep"), "tp"), check_vma=False
    )
```

```python
import functools

import jax
import jax.numpy as jnp
from jax import lax
from jax.experimental import pallas as pl
from jax.experimental.pallas import tpu as pltpu
from jax.sharding import PartitionSpec as P

D = 3584
FF = 2560
WAVE = 2
MEMBERS = 8
GROUP_EP = 4
TOK_G = 512
CAP = 128
LANES = 128
EXTRA = 16


def as_sent(array):

    def short(part):
        return part.astype(jnp.bfloat16) if part.dtype == jnp.float32 else part

    return jax.tree.map(short, array)


def swapped(array, axis, distance):
    return lax.ppermute(array, axis, [(i, i ^ 1 << distance) for i in range(lax.axis_size(axis))])


def dispatch_slots(expert_ids, gate_values, live_count, expert):
    row_index = jnp.arange(TOK_G, dtype=jnp.int32)
    live_rows = row_index < live_count
    hit_mask = expert_ids == expert
    selected = jnp.logical_and(jnp.any(hit_mask, axis=1), live_rows)
    row_weight = jnp.sum(jnp.where(hit_mask, gate_values, jnp.float32(0.0)), axis=1)
    position = jnp.cumsum(selected.astype(jnp.int32)) - 1
    slot_index = jnp.arange(CAP, dtype=jnp.int32)
    slot_match = jnp.logical_and(position[None, :] == slot_index[:, None], selected[None, :])
    slot_rows = jnp.sum(jnp.where(slot_match, row_index[None, :], 0), axis=1)
    slot_valid = jnp.any(slot_match, axis=1)
    slot_weight = jnp.where(slot_valid, row_weight[slot_rows], jnp.float32(0.0))
    return (slot_rows, slot_weight)


def travelling(tokens, expert_ids, gate_values, group_counts, gate_weight, up_weight, down_weight):
    ep_index = lax.axis_index("ep")
    slice_width = FF // MEMBERS
    group_bits = GROUP_EP.bit_length() - 1
    weight_stack = jnp.stack([gate_weight, up_weight, down_weight])
    rows_held = weight_stack.shape[1]
    pieces = weight_stack.shape[2] // slice_width
    slice_blocks = weight_stack.reshape(3, rows_held, pieces, slice_width).transpose(0, 2, 1, 3)
    fan_out = lax.axis_size("ep") // pieces
    outgoing = jnp.tile(slice_blocks, (1, fan_out, 1, 1))
    arrived = lax.all_to_all(outgoing, "ep", split_axis=1, concat_axis=1, tiled=True)
    columns = arrived.reshape(3, -1, slice_width)
    features = lax.all_gather(tokens, "tp", axis=1, tiled=True)
    group_data = (features, expert_ids, gate_values)
    for bit_level in range(group_bits):
        received = jax.tree.map(
            lambda part, own: part.astype(own.dtype),
            swapped(as_sent(group_data), "ep", bit_level),
            group_data,
        )
        upper_half = ep_index >> bit_level & 1 == 1
        group_data = tuple(
            (
                jnp.where(
                    upper_half, jnp.concatenate([other, own], 0), jnp.concatenate([own, other], 0)
                )
                for own, other in zip(group_data, received)
            )
        )
    group_tokens, group_ids, group_gates = group_data
    live_count = lax.dynamic_index_in_dim(group_counts, ep_index // GROUP_EP, keepdims=False)
    partials = jnp.zeros((group_tokens.shape[0], D), jnp.float32)
    for expert in range(WAVE):
        slot_rows, slot_weight = dispatch_slots(group_ids, group_gates, live_count, expert)
        expert_rows = group_tokens[slot_rows]
        gate_cols = columns[0, expert * D : (expert + 1) * D]
        up_cols = columns[1, expert * D : (expert + 1) * D]
        down_cols = columns[2, expert * D : (expert + 1) * D]
        gate_act = jnp.dot(expert_rows, gate_cols, preferred_element_type=jnp.float32)
        up_act = jnp.dot(expert_rows, up_cols, preferred_element_type=jnp.float32)
        hidden = (jax.nn.silu(gate_act) * up_act).astype(jnp.bfloat16)
        projected = lax.dot_general(
            hidden, down_cols, (((1,), (1,)), ((), ())), preferred_element_type=jnp.float32
        )
        partials = partials.at[slot_rows].add(slot_weight[:, None] * projected)
    rounded = lax.optimization_barrier(partials.astype(jnp.bfloat16)).astype(jnp.float32)
    halved = lax.psum_scatter(
        rounded.astype(jnp.bfloat16), "tp", scatter_dimension=1, tiled=True
    ).astype(jnp.float32)
    for bit_level in reversed(range(group_bits)):
        paired_up = halved.reshape(2, -1, halved.shape[1])
        upper_half = ep_index >> bit_level & 1 == 1
        kept_part = jnp.where(upper_half, paired_up[1], paired_up[0])
        sent_part = jnp.where(upper_half, paired_up[0], paired_up[1])
        halved = kept_part + swapped(sent_part.astype(jnp.bfloat16), "ep", bit_level).astype(
            sent_part.dtype
        )
    return halved.astype(jnp.bfloat16)


def place_of(members):
    ep = lax.axis_index("ep")
    return ep // members, ep % members, lax.axis_index("tp")


def is_side(own_side, members):
    square, _, core = place_of(members)
    return (square == core) == own_side


def piece_copies(held, came, turn, members, destination, sem):
    _, member, core = place_of(members)
    width = destination.shape[1]
    per_half = held.shape[1] // width
    block = jnp.bitwise_xor(member, turn)
    columns = pl.ds(pl.multiple_of(block % per_half * width, LANES), width)
    is_held = block // per_half == core
    return is_held, [
        pltpu.make_async_copy(half.at[:, columns], destination, sem) for half in (held, came)
    ]


def start_piece(is_held, copies):
    @pl.when(is_held)
    def _():
        copies[0].start()

    @pl.when(jnp.logical_not(is_held))
    def _():
        copies[1].start()


def pack_kernel(members, counts, held, came, expert_ids, gate_values, *refs):
    outs, (table_ref, sem) = refs[:members], refs[members:]
    square, member, _ = place_of(members)
    rows = held.shape[0]
    pieces = [
        piece_copies(held, came, turn, members, out.at[:rows], sem.at[0, turn])
        for turn, out in enumerate(outs)
    ]
    for piece in pieces:
        start_piece(*piece)
    is_live = lax.broadcasted_iota(jnp.int32, (1, rows), 1) < counts[square] - member * rows
    ids, gates = expert_ids[...], gate_values[...]
    place = lax.broadcasted_iota(jnp.int32, (EXTRA, rows), 0)
    rest = jnp.zeros((EXTRA, rows), jnp.float32)
    for n, expert in enumerate((square, WAVE - 1 - square)):
        named = jnp.sum(jnp.where(ids == expert, gates, 0.0), axis=0, keepdims=True)
        rest = jnp.where(place == n, jnp.where(is_live, named, 0.0), rest)
    table_ref[...] = jnp.zeros(table_ref.shape, table_ref.dtype)
    for term in range(3):
        part = rest.astype(jnp.bfloat16)
        rest = rest - part.astype(jnp.float32)
        table_ref[:, term * rows : (term + 1) * rows] = part
    tables = [
        pltpu.make_async_copy(table_ref, out.at[rows:], sem.at[1, turn])
        for turn, out in enumerate(outs)
    ]
    for copy in tables:
        copy.start()
    for copy in [copies[0] for _, copies in pieces] + tables:
        copy.wait()


def routing_of(block, rows):
    extra = block[rows:, : 3 * LANES].astype(jnp.float32)
    return extra[:, :LANES] + extra[:, LANES : 2 * LANES] + extra[:, 2 * LANES :]


def compact_kernel(*refs):
    blocks, (own_ref, other_ref, place_ref, weight_ref) = refs[:-4], refs[-4:]
    member = place_of(len(blocks))[1]
    slots = own_ref.shape[0]
    rows = blocks[0].shape[0] - EXTRA
    before = lax.broadcasted_iota(jnp.int32, (rows, rows), 0)
    after = lax.broadcasted_iota(jnp.int32, (rows, rows), 1)
    upto = (before <= after).astype(jnp.float32).astype(jnp.bfloat16)
    slot = lax.broadcasted_iota(jnp.int32, (slots, rows), 0)
    total = jnp.zeros((2 * slots, own_ref.shape[1]), jnp.float32)
    weights = [routing_of(block, rows) for block in blocks]
    counts = [
        jnp.dot(
            (weight > 0.0).astype(jnp.float32).astype(jnp.bfloat16),
            upto,
            preferred_element_type=jnp.float32,
        )
        for weight in weights
    ]
    for turn, block in enumerate(blocks):
        weight, count = weights[turn], counts[turn]
        for before, earlier in enumerate(counts):
            if before != turn:
                ahead = jnp.bitwise_xor(member, before) < jnp.bitwise_xor(member, turn)
                count = count + jnp.where(ahead, earlier[:, rows - 1 :], 0.0)
        place = jnp.where(weight > 0.0, count - 1.0, -1.0).astype(jnp.int32)
        pick = jnp.concatenate(
            [(slot == place[e : e + 1, :]).astype(jnp.float32) for e in range(WAVE)], 0
        ).astype(jnp.bfloat16)
        total = total + jnp.dot(pick, block[:rows, :], preferred_element_type=jnp.float32)
        place_ref[turn] = place[:8]
        weight_ref[turn] = weight[:8]
    own_ref[...] = total[:slots].astype(own_ref.dtype)
    other_ref[...] = total[slots:].astype(other_ref.dtype)


def spread_kernel(place_ref, weight_ref, _, pick_ref, column_ref):
    rows = place_ref.shape[2]
    slot = lax.broadcasted_iota(jnp.int32, (CAP, rows), 0)
    for turn in range(place_ref.shape[0]):
        place, weight = place_ref[turn], weight_ref[turn]
        for e in range(WAVE):
            pick = (slot == place[e : e + 1, :]).astype(jnp.float32)
            pick_ref[turn, :, e * CAP : (e + 1) * CAP] = pick.T.astype(pick_ref.dtype)
        table = jnp.where(slot == 0, weight[0:1, :], jnp.where(slot == 1, weight[1:2, :], 0.0))
        column_ref[turn] = table.T


def with_piece(members, turn, width, held, came, use):
    _, member, core = place_of(members)
    per_half = held[0].shape[1] // width
    block = jnp.bitwise_xor(member, turn)
    columns = pl.ds(pl.multiple_of(block % per_half * width, LANES), width)

    @pl.when(block // per_half == core)
    def _():
        use([half.at[:, columns] for half in held])

    @pl.when(block // per_half != core)
    def _():
        use([half.at[:, columns] for half in came])


def part_kernel(members, own_side, turn, rows_ref, *refs):
    held, came, out_ref = refs[:2], refs[2:4], refs[-1]
    width = out_ref.shape[1] // 2

    def use(weights):
        for n, weight in enumerate(weights):
            out_ref[:, n * width : (n + 1) * width] = jnp.dot(
                rows_ref[...], weight[...], preferred_element_type=jnp.float32
            ).astype(out_ref.dtype)

    @pl.when(is_side(own_side, members))
    def _():
        with_piece(members, turn, width, held, came, use)


def hidden_kernel(members, own_side, *refs):
    parts, out_ref = refs[:members], refs[-1]
    width = out_ref.shape[1]

    @pl.when(is_side(own_side, members))
    def _():
        gate, up = (
            sum(part[:, n * width : (n + 1) * width].astype(jnp.float32) for part in parts)
            for n in range(2)
        )
        out_ref[...] = (gate / (1.0 + jnp.exp(-gate)) * up).astype(out_ref.dtype)


def down_kernel(members, own_side, *refs):
    hidden, (held, came), (out_ref, total_ref) = refs[:members], refs[members : members + 2], refs[-2:]

    def use_turn(turn):
        def use(weights):
            product = lax.dot_general(
                hidden[turn][...],
                weights[0][...],
                (((1,), (1,)), ((), ())),
                preferred_element_type=jnp.float32,
            )
            total_ref[...] = product if turn == 0 else total_ref[...] + product

        return use

    @pl.when(is_side(own_side, members))
    def _():
        for turn in range(members):
            with_piece(members, turn, hidden[0].shape[1], [held], [came], use_turn(turn))
        out_ref[...] = total_ref[...].astype(out_ref.dtype)


def expand_kernel(own_ref, other_ref, pick_ref, column_ref, *outs):
    for turn, out in enumerate(outs):
        total = None
        for e, ref in enumerate((own_ref, other_ref)):
            chosen = jnp.dot(
                pick_ref[turn, :, e * CAP : (e + 1) * CAP],
                ref[...],
                preferred_element_type=jnp.float32,
            )
            part = column_ref[turn, :, e : e + 1] * chosen
            total = part if total is None else total + part
        out[...] = total.astype(out.dtype)


VMEM = pl.BlockSpec(memory_space=pltpu.VMEM)
SMEM = pl.BlockSpec(memory_space=pltpu.SMEM)
HBM = pl.BlockSpec(memory_space=pltpu.HBM)


def call(kernel, name, outs, specs, scratch=(), mib=8, space=VMEM, flops=0):
    return pl.pallas_call(
        kernel,
        out_shape=[jax.ShapeDtypeStruct(shape, dtype) for shape, dtype in outs],
        in_specs=specs,
        out_specs=[space] * len(outs),
        scratch_shapes=list(scratch),
        compiler_params=pltpu.CompilerParams(vmem_limit_bytes=mib * 1024 * 1024),
        cost_estimate=pl.CostEstimate(flops=flops, bytes_accessed=0, transcendentals=0),
        name=name,
    )


def moved(array, ep_size, tp_size, target, full=False):
    targets = {(e, t): target(e, t) for e in range(ep_size) for t in range(tp_size)}
    used = set(targets.values())
    pairs = []
    for (e, t), to in targets.items():
        if to is None and full:
            (to,) = [(e, core) for core in range(tp_size) if (e, core) not in used]
        if to is not None:
            pairs.append((e * tp_size + t, to[0] * tp_size + to[1]))
    return lax.ppermute(array, ("ep", "tp"), pairs)


def resting(
    tokens, expert_ids, gate_values, group_counts, gate_weight, up_weight, down_weight
):
    ep_size, tp_size = lax.axis_size("ep"), lax.axis_size("tp")
    ep, core = lax.axis_index("ep"), lax.axis_index("tp")
    rows = tokens.shape[0]
    members = TOK_G // rows
    per_core = members // tp_size
    member = ep % members
    thick = gate_weight.shape[0]
    width = tp_size * gate_weight.shape[1] // members
    bf16, f32 = jnp.bfloat16, jnp.float32
    send = functools.partial(moved, ep_size=ep_size, tp_size=tp_size)
    far_first = [members - 1 - n for n in range(members - 1)]

    def partner(turn, own_side):
        return lambda e, t: (e ^ turn, t) if (t == e // members) == own_side else None

    def across(from_own):
        return lambda e, t: (
            ((e + members) % ep_size, t) if (t == e // members) == from_own else None
        )

    other_half = [(t, tp_size - 1 - t) for t in range(tp_size)]
    tokens_came = lax.ppermute(tokens, "tp", other_half)
    packed = call(
        functools.partial(pack_kernel, members),
        "pack",
        [((rows + EXTRA, thick), bf16)] * members,
        [SMEM, HBM, HBM, VMEM, VMEM],
        [pltpu.VMEM((EXTRA, thick), bf16), pltpu.SemaphoreType.DMA((2, members))],
        space=HBM,
    )(group_counts, tokens, tokens_came, expert_ids.T, gate_values.T)
    arrived = {0: packed[0]}
    for turn in far_first:
        arrived[turn] = send(packed[turn], target=partner(turn, True))
    gate_came, up_came, down_came = (
        lax.ppermute(weight, "tp", other_half) for weight in (gate_weight, up_weight, down_weight)
    )

    own_rows, other_rows, place, weight = call(
        compact_kernel,
        "compact",
        [
            ((CAP, thick), bf16),
            ((CAP, thick), bf16),
            ((members, 8, rows), jnp.int32),
            ((members, 8, rows), f32),
        ],
        [VMEM] * members,
    )(*[arrived[turn] for turn in range(members)])
    came_rows = send(other_rows, target=across(True), full=True)

    def parts_of(own_side, slot_rows, after):
        parts, last = {}, list(after)
        for turn in far_first + [0]:
            parts[turn] = call(
                functools.partial(part_kernel, members, own_side, turn),
                "part",
                [((CAP, 2 * width), bf16 if turn else f32)],
                [VMEM] * 5 + [HBM] * len(last),
                mib=16,
                flops=4 * CAP * thick * width,
            )(slot_rows, gate_weight, up_weight, gate_came, up_came, *last)[0]
            last = [parts[turn]]
        came = [send(parts[turn], target=partner(turn, own_side)) for turn in far_first]
        return [parts[0]] + came

    def hidden_of(own_side, parts, after):
        hidden = call(
            functools.partial(hidden_kernel, members, own_side),
            "hidden",
            [((CAP, width), bf16)],
            [VMEM] * members + [HBM],
        )(*parts, after)[0]
        came = {turn: send(hidden, target=partner(turn, own_side)) for turn in far_first}
        return [hidden] + [came[turn] for turn in range(1, members)]

    own_parts = parts_of(True, own_rows, [])
    other_parts = parts_of(False, came_rows, [own_parts[0]])
    own_hidden = hidden_of(True, own_parts, other_parts[0])
    other_hidden = hidden_of(False, other_parts, own_hidden[0])

    def down_of(own_side, hidden, after):
        return call(
            functools.partial(down_kernel, members, own_side),
            "down",
            [((CAP, thick), bf16)],
            [VMEM] * (members + 2) + [HBM],
            [pltpu.VMEM((CAP, thick), f32)],
            16,
        )(*hidden, down_weight, down_came, after)[0]

    own_projected = down_of(True, own_hidden, other_hidden[0])
    other_projected = down_of(False, other_hidden, own_projected)
    came_projected = send(other_projected, target=across(False), full=True)

    pick, column = call(
        spread_kernel,
        "spread",
        [((members, rows, WAVE * CAP), bf16), ((members, rows, LANES), f32)],
        [VMEM] * 2 + [HBM],
    )(place, weight, other_parts[0])
    spread = call(
        expand_kernel, "expand", [((rows, thick), bf16)] * members, [VMEM] * 4
    )(own_projected, came_projected, pick, column)

    def back(turn):
        def target(e, t):
            return (e ^ turn, e % members // per_core) if e // members == t else None

        return target

    returned = {
        turn: send(spread[turn], target=back(turn), full=True) for turn in far_first + [0]
    }
    low = core == member // per_core
    even, odd = (jnp.where(low, returned[n], returned[n + per_core]) for n in range(per_core))
    swap = member % per_core == 1
    return jnp.concatenate([jnp.where(swap, odd, even), jnp.where(swap, even, odd)], axis=1)


def shards(tokens, expert_ids, gate_values, group_counts, gate_weight, up_weight, down_weight):
    ep_size, tp_size = lax.axis_size("ep"), lax.axis_size("tp")
    members = TOK_G // tokens.shape[0]
    rests = ep_size == WAVE * members and tp_size == WAVE and members == 2 * tp_size
    return (resting if rests else travelling)(
        tokens, expert_ids, gate_values, group_counts, gate_weight, up_weight, down_weight
    )


def solution(mesh):
    placed = (
        P(("rep", "ep"), "tp"),
        P(("rep", "ep"), None),
        P(("rep", "ep"), None),
        P("rep"),
        P(("rep", "ep"), "tp"),
        P(("rep", "ep"), "tp"),
        P(("rep", "ep"), "tp"),
    )
    return jax.shard_map(
        shards, mesh=mesh, in_specs=placed, out_specs=P(("rep", "ep"), "tp"), check_vma=False
    )
```

```python
import functools

import jax
import jax.numpy as jnp
from jax import lax
from jax.experimental import pallas as pl
from jax.experimental.pallas import tpu as pltpu
from jax.sharding import PartitionSpec as P


D = 3584
FF = 2560
WAVE = 2
MEMBERS = 8
GROUP_EP = 4
TOK_G = 512
CAP = 128
LANES = 128
EXTRA = 16


def as_sent(array):

    def short(part):
        return part.astype(jnp.bfloat16) if part.dtype == jnp.float32 else part

    return jax.tree.map(short, array)


def swapped(array, axis, distance):
    return lax.ppermute(array, axis, [(i, i ^ 1 << distance) for i in range(lax.axis_size(axis))])


def dispatch_slots(expert_ids, gate_values, live_count, expert):
    row_index = jnp.arange(TOK_G, dtype=jnp.int32)
    live_rows = row_index < live_count
    hit_mask = expert_ids == expert
    selected = jnp.logical_and(jnp.any(hit_mask, axis=1), live_rows)
    row_weight = jnp.sum(jnp.where(hit_mask, gate_values, jnp.float32(0.0)), axis=1)
    position = jnp.cumsum(selected.astype(jnp.int32)) - 1
    slot_index = jnp.arange(CAP, dtype=jnp.int32)
    slot_match = jnp.logical_and(position[None, :] == slot_index[:, None], selected[None, :])
    slot_rows = jnp.sum(jnp.where(slot_match, row_index[None, :], 0), axis=1)
    slot_valid = jnp.any(slot_match, axis=1)
    slot_weight = jnp.where(slot_valid, row_weight[slot_rows], jnp.float32(0.0))
    return (slot_rows, slot_weight)


def travelling(tokens, expert_ids, gate_values, group_counts, gate_weight, up_weight, down_weight):
    ep_index = lax.axis_index("ep")
    slice_width = FF // MEMBERS
    group_bits = GROUP_EP.bit_length() - 1
    weight_stack = jnp.stack([gate_weight, up_weight, down_weight])
    rows_held = weight_stack.shape[1]
    pieces = weight_stack.shape[2] // slice_width
    slice_blocks = weight_stack.reshape(3, rows_held, pieces, slice_width).transpose(0, 2, 1, 3)
    fan_out = lax.axis_size("ep") // pieces
    outgoing = jnp.tile(slice_blocks, (1, fan_out, 1, 1))
    arrived = lax.all_to_all(outgoing, "ep", split_axis=1, concat_axis=1, tiled=True)
    columns = arrived.reshape(3, -1, slice_width)
    features = lax.all_gather(tokens, "tp", axis=1, tiled=True)
    group_data = (features, expert_ids, gate_values)
    for bit_level in range(group_bits):
        received = jax.tree.map(
            lambda part, own: part.astype(own.dtype),
            swapped(as_sent(group_data), "ep", bit_level),
            group_data,
        )
        upper_half = ep_index >> bit_level & 1 == 1
        group_data = tuple(
            (
                jnp.where(
                    upper_half, jnp.concatenate([other, own], 0), jnp.concatenate([own, other], 0)
                )
                for own, other in zip(group_data, received)
            )
        )
    group_tokens, group_ids, group_gates = group_data
    live_count = lax.dynamic_index_in_dim(group_counts, ep_index // GROUP_EP, keepdims=False)
    partials = jnp.zeros((group_tokens.shape[0], D), jnp.float32)
    for expert in range(WAVE):
        slot_rows, slot_weight = dispatch_slots(group_ids, group_gates, live_count, expert)
        expert_rows = group_tokens[slot_rows]
        gate_cols = columns[0, expert * D : (expert + 1) * D]
        up_cols = columns[1, expert * D : (expert + 1) * D]
        down_cols = columns[2, expert * D : (expert + 1) * D]
        gate_act = jnp.dot(expert_rows, gate_cols, preferred_element_type=jnp.float32)
        up_act = jnp.dot(expert_rows, up_cols, preferred_element_type=jnp.float32)
        hidden = (jax.nn.silu(gate_act) * up_act).astype(jnp.bfloat16)
        projected = lax.dot_general(
            hidden, down_cols, (((1,), (1,)), ((), ())), preferred_element_type=jnp.float32
        )
        partials = partials.at[slot_rows].add(slot_weight[:, None] * projected)
    rounded = lax.optimization_barrier(partials.astype(jnp.bfloat16)).astype(jnp.float32)
    halved = lax.psum_scatter(
        rounded.astype(jnp.bfloat16), "tp", scatter_dimension=1, tiled=True
    ).astype(jnp.float32)
    for bit_level in reversed(range(group_bits)):
        paired_up = halved.reshape(2, -1, halved.shape[1])
        upper_half = ep_index >> bit_level & 1 == 1
        kept_part = jnp.where(upper_half, paired_up[1], paired_up[0])
        sent_part = jnp.where(upper_half, paired_up[0], paired_up[1])
        halved = kept_part + swapped(sent_part.astype(jnp.bfloat16), "ep", bit_level).astype(
            sent_part.dtype
        )
    return halved.astype(jnp.bfloat16)


def place_of(members):
    ep = lax.axis_index("ep")
    return ep // members, ep % members, lax.axis_index("tp")


def is_side(own_side, members):
    square, _, core = place_of(members)
    return (square == core) == own_side


def piece_copies(held, came, turn, members, destination, sem):
    _, member, core = place_of(members)
    width = destination.shape[1]
    per_half = held.shape[1] // width
    block = jnp.bitwise_xor(member, turn)
    columns = pl.ds(pl.multiple_of(block % per_half * width, LANES), width)
    is_held = block // per_half == core
    return is_held, [
        pltpu.make_async_copy(half.at[:, columns], destination, sem) for half in (held, came)
    ]


def start_piece(is_held, copies):
    @pl.when(is_held)
    def _():
        copies[0].start()

    @pl.when(jnp.logical_not(is_held))
    def _():
        copies[1].start()


def route_kernel(members, counts, expert_ids, gate_values, tokens, table_ref):
    square, member, _ = place_of(members)
    rows = expert_ids.shape[1]
    is_live = lax.broadcasted_iota(jnp.int32, (1, rows), 1) < counts[square] - member * rows
    ids, gates = expert_ids[...], gate_values[...]
    place = lax.broadcasted_iota(jnp.int32, (EXTRA, rows), 0)
    rest = jnp.zeros((EXTRA, rows), jnp.float32)
    for n, expert in enumerate((square, WAVE - 1 - square)):
        named = jnp.sum(jnp.where(ids == expert, gates, 0.0), axis=0, keepdims=True)
        rest = jnp.where(place == n, jnp.where(is_live, named, 0.0), rest)
    table_ref[...] = jnp.zeros(table_ref.shape, table_ref.dtype)
    for term in range(3):
        part = rest.astype(jnp.bfloat16)
        rest = rest - part.astype(jnp.float32)
        table_ref[:, term * rows : (term + 1) * rows] = part


def pack_kernel(members, table_ref, held, came, *refs):
    outs, sem = refs[:members], refs[members]
    rows = held.shape[0]
    pieces = [
        piece_copies(held, came, turn, members, out.at[:rows], sem.at[0, turn])
        for turn, out in enumerate(outs)
    ]
    tables = [
        pltpu.make_async_copy(table_ref, out.at[rows:], sem.at[1, turn])
        for turn, out in enumerate(outs)
    ]
    for piece in pieces:
        start_piece(*piece)
    for copy in tables:
        copy.start()
    for copy in [copies[0] for _, copies in pieces] + tables:
        copy.wait()


def routing_of(block, rows):
    extra = block[rows:, : 3 * LANES].astype(jnp.float32)
    return extra[:, :LANES] + extra[:, LANES : 2 * LANES] + extra[:, 2 * LANES :]


def compact_kernel(*refs):
    blocks, (own_ref, other_ref, place_ref, weight_ref) = refs[:-4], refs[-4:]
    member = place_of(len(blocks))[1]
    slots = own_ref.shape[0]
    rows = blocks[0].shape[0] - EXTRA
    before = lax.broadcasted_iota(jnp.int32, (rows, rows), 0)
    after = lax.broadcasted_iota(jnp.int32, (rows, rows), 1)
    upto = (before <= after).astype(jnp.float32).astype(jnp.bfloat16)
    slot = lax.broadcasted_iota(jnp.int32, (slots, rows), 0)
    total = jnp.zeros((2 * slots, own_ref.shape[1]), jnp.float32)
    weights = [routing_of(block, rows) for block in blocks]
    counts = [
        jnp.dot(
            (weight > 0.0).astype(jnp.float32).astype(jnp.bfloat16),
            upto,
            preferred_element_type=jnp.float32,
        )
        for weight in weights
    ]
    for turn, block in enumerate(blocks):
        weight, count = weights[turn], counts[turn]
        for before, earlier in enumerate(counts):
            if before != turn:
                ahead = jnp.bitwise_xor(member, before) < jnp.bitwise_xor(member, turn)
                count = count + jnp.where(ahead, earlier[:, rows - 1 :], 0.0)
        place = jnp.where(weight > 0.0, count - 1.0, -1.0).astype(jnp.int32)
        pick = jnp.concatenate(
            [(slot == place[e : e + 1, :]).astype(jnp.float32) for e in range(WAVE)], 0
        ).astype(jnp.bfloat16)
        total = total + jnp.dot(pick, block[:rows, :], preferred_element_type=jnp.float32)
        place_ref[turn] = place[:8]
        weight_ref[turn] = weight[:8]
    own_ref[...] = total[:slots].astype(own_ref.dtype)
    other_ref[...] = total[slots:].astype(other_ref.dtype)


def spread_kernel(place_ref, weight_ref, _, pick_ref, column_ref):
    rows = place_ref.shape[2]
    slot = lax.broadcasted_iota(jnp.int32, (CAP, rows), 0)
    for turn in range(place_ref.shape[0]):
        place, weight = place_ref[turn], weight_ref[turn]
        for e in range(WAVE):
            pick = (slot == place[e : e + 1, :]).astype(jnp.float32)
            pick_ref[turn, :, e * CAP : (e + 1) * CAP] = pick.T.astype(pick_ref.dtype)
        table = jnp.where(slot == 0, weight[0:1, :], jnp.where(slot == 1, weight[1:2, :], 0.0))
        column_ref[turn] = table.T


def with_piece(members, turn, width, held, came, use):
    _, member, core = place_of(members)
    per_half = held[0].shape[1] // width
    block = jnp.bitwise_xor(member, turn)
    columns = pl.ds(pl.multiple_of(block % per_half * width, LANES), width)

    @pl.when(block // per_half == core)
    def _():
        use([half.at[:, columns] for half in held])

    @pl.when(block // per_half != core)
    def _():
        use([half.at[:, columns] for half in came])


def part_kernel(members, own_side, turn, rows_ref, *refs):
    held, came, out_ref = refs[:2], refs[2:4], refs[-1]
    width = out_ref.shape[1] // 2

    def use(weights):
        for n, weight in enumerate(weights):
            out_ref[:, n * width : (n + 1) * width] = jnp.dot(
                rows_ref[...], weight[...], preferred_element_type=jnp.float32
            ).astype(out_ref.dtype)

    @pl.when(is_side(own_side, members))
    def _():
        with_piece(members, turn, width, held, came, use)


def hidden_kernel(members, own_side, *refs):
    parts, out_ref = refs[:members], refs[-1]
    width = out_ref.shape[1]

    @pl.when(is_side(own_side, members))
    def _():
        gate, up = (
            sum(part[:, n * width : (n + 1) * width].astype(jnp.float32) for part in parts)
            for n in range(2)
        )
        out_ref[...] = (gate / (1.0 + jnp.exp(-gate)) * up).astype(out_ref.dtype)


def down_kernel(members, own_side, *refs):
    hidden, (held, came), (out_ref, total_ref) = refs[:members], refs[members : members + 2], refs[-2:]

    def use_turn(turn):
        def use(weights):
            product = lax.dot_general(
                hidden[turn][...],
                weights[0][...],
                (((1,), (1,)), ((), ())),
                preferred_element_type=jnp.float32,
            )
            total_ref[...] = product if turn == 0 else total_ref[...] + product

        return use

    @pl.when(is_side(own_side, members))
    def _():
        for turn in range(members):
            with_piece(members, turn, hidden[0].shape[1], [held], [came], use_turn(turn))
        out_ref[...] = total_ref[...].astype(out_ref.dtype)


def expand_kernel(own_ref, other_ref, pick_ref, column_ref, *outs):
    for turn, out in enumerate(outs):
        total = None
        for e, ref in enumerate((own_ref, other_ref)):
            chosen = jnp.dot(
                pick_ref[turn, :, e * CAP : (e + 1) * CAP],
                ref[...],
                preferred_element_type=jnp.float32,
            )
            part = column_ref[turn, :, e : e + 1] * chosen
            total = part if total is None else total + part
        out[...] = total.astype(out.dtype)


VMEM = pl.BlockSpec(memory_space=pltpu.VMEM)
SMEM = pl.BlockSpec(memory_space=pltpu.SMEM)
HBM = pl.BlockSpec(memory_space=pltpu.HBM)


def call(kernel, outs, specs, scratch=(), mib=8, space=VMEM, flops=0):
    return pl.pallas_call(
        kernel,
        out_shape=[jax.ShapeDtypeStruct(shape, dtype) for shape, dtype in outs],
        in_specs=specs,
        out_specs=[space] * len(outs),
        scratch_shapes=list(scratch),
        compiler_params=pltpu.CompilerParams(vmem_limit_bytes=mib * 1024 * 1024),
        cost_estimate=pl.CostEstimate(flops=flops, bytes_accessed=0, transcendentals=0),
    )


def moved(array, ep_size, tp_size, target):
    targets = {(e, t): target(e, t) for e in range(ep_size) for t in range(tp_size)}
    used = set(targets.values())
    pairs = []
    for (e, t), to in targets.items():
        if to is None:
            (to,) = [(e, core) for core in range(tp_size) if (e, core) not in used]
        pairs.append((e * tp_size + t, to[0] * tp_size + to[1]))
    return lax.ppermute(array, ("ep", "tp"), pairs)


def resting(
    tokens, expert_ids, gate_values, group_counts, gate_weight, up_weight, down_weight
):
    ep_size, tp_size = lax.axis_size("ep"), lax.axis_size("tp")
    ep, core = lax.axis_index("ep"), lax.axis_index("tp")
    rows = tokens.shape[0]
    members = TOK_G // rows
    per_core = members // tp_size
    member = ep % members
    thick = gate_weight.shape[0]
    width = tp_size * gate_weight.shape[1] // members
    bf16, f32 = jnp.bfloat16, jnp.float32
    send = functools.partial(moved, ep_size=ep_size, tp_size=tp_size)
    far_first = [members - 1 - n for n in range(members - 1)]

    def crosswise(turn, from_own):
        return lambda e, t: (
            (e ^ turn, tp_size - 1 - t) if (t == e // members) == from_own else None
        )

    def across(from_own):
        return lambda e, t: (
            ((e + members) % ep_size, t) if (t == e // members) == from_own else None
        )

    other_half = [(t, tp_size - 1 - t) for t in range(tp_size)]
    tokens_came = lax.ppermute(tokens, "tp", other_half)
    (table,) = call(
        functools.partial(route_kernel, members), [((EXTRA, thick), bf16)], [SMEM, VMEM, VMEM, HBM]
    )(group_counts, expert_ids.T, gate_values.T, tokens)
    packed = call(
        functools.partial(pack_kernel, members),
        [((rows + EXTRA, thick), bf16)] * members,
        [VMEM, HBM, HBM],
        [pltpu.SemaphoreType.DMA((2, members))],
        space=HBM,
    )(table, tokens, tokens_came)
    arrived = {0: packed[0]}
    for turn in far_first:
        arrived[turn] = send(packed[turn], target=crosswise(turn, False))
    weights_came = []
    for weight in (gate_weight, up_weight, down_weight):
        weights_came.append(lax.ppermute(weight, "tp", other_half))
    gate_came, up_came, down_came = weights_came

    own_rows, other_rows, place, weight = call(
        compact_kernel,
        [
            ((CAP, thick), bf16),
            ((CAP, thick), bf16),
            ((members, 8, rows), jnp.int32),
            ((members, 8, rows), f32),
        ],
        [VMEM] * members,
    )(*[arrived[turn] for turn in range(members)])
    came_rows = send(other_rows, target=across(True))

    def parts_of(own_side, slot_rows, after):
        parts, last = {}, list(after)
        for turn in far_first + [0]:
            parts[turn] = call(
                functools.partial(part_kernel, members, own_side, turn),
                [((CAP, 2 * width), bf16)],
                [VMEM] * 5 + [HBM] * len(last),
                mib=16,
                flops=4 * CAP * thick * width,
            )(slot_rows, gate_weight, up_weight, gate_came, up_came, *last)[0]
            last = [parts[turn]]
        came = []
        for turn in far_first + [0]:
            came.append(send(parts[turn], target=crosswise(turn, own_side)))
        return came, parts[0]

    def hidden_of(own_side, parts, after):
        hidden = call(
            functools.partial(hidden_kernel, members, not own_side),
            [((CAP, width), bf16)],
            [VMEM] * members + [HBM],
        )(*parts, after)[0]
        came = {}
        for turn in far_first + [0]:
            came[turn] = send(hidden, target=crosswise(turn, not own_side))
        return [came[turn] for turn in range(members)], hidden

    own_parts, own_last = parts_of(True, own_rows, [])
    other_parts, other_last = parts_of(False, came_rows, [own_last])
    own_hidden, own_last = hidden_of(True, own_parts, other_last)
    other_hidden, other_last = hidden_of(False, other_parts, own_last)

    def down_of(own_side, hidden, after):
        return call(
            functools.partial(down_kernel, members, own_side),
            [((CAP, thick), bf16)],
            [VMEM] * (members + 2) + [HBM],
            [pltpu.VMEM((CAP, thick), f32)],
            16,
        )(*hidden, down_weight, down_came, after)[0]

    own_projected = down_of(True, own_hidden, other_last)
    other_projected = down_of(False, other_hidden, own_projected)
    came_projected = send(other_projected, target=across(False))

    pick, column = call(
        spread_kernel,
        [((members, rows, WAVE * CAP), bf16), ((members, rows, LANES), f32)],
        [VMEM] * 2 + [HBM],
    )(place, weight, own_last)
    spread = call(
        expand_kernel, [((rows, thick), bf16)] * members, [VMEM] * 4
    )(own_projected, came_projected, pick, column)

    def back(turn):
        def target(e, t):
            return (e ^ turn, e % members // per_core) if e // members == t else None

        return target

    returned = {}
    for turn in far_first + [0]:
        returned[turn] = send(spread[turn], target=back(turn))
    low = core == member // per_core
    even, odd = (jnp.where(low, returned[n], returned[n + per_core]) for n in range(per_core))
    swap = member % per_core == 1
    return jnp.concatenate([jnp.where(swap, odd, even), jnp.where(swap, even, odd)], axis=1)


def shards(tokens, expert_ids, gate_values, group_counts, gate_weight, up_weight, down_weight):
    ep_size, tp_size = lax.axis_size("ep"), lax.axis_size("tp")
    members = TOK_G // tokens.shape[0]
    rests = ep_size == WAVE * members and tp_size == WAVE and members == 2 * tp_size
    return (resting if rests else travelling)(
        tokens, expert_ids, gate_values, group_counts, gate_weight, up_weight, down_weight
    )


def solution(mesh):
    placed = (
        P(("rep", "ep"), "tp"),
        P(("rep", "ep"), None),
        P(("rep", "ep"), None),
        P("rep"),
        P(("rep", "ep"), "tp"),
        P(("rep", "ep"), "tp"),
        P(("rep", "ep"), "tp"),
    )
    return jax.shard_map(
        shards, mesh=mesh, in_specs=placed, out_specs=P(("rep", "ep"), "tp"), check_vma=False
    )
```

```python
import functools

import jax
import jax.numpy as jnp
from jax import lax
from jax.experimental import pallas as pl
from jax.experimental.pallas import tpu as pltpu
from jax.sharding import PartitionSpec as P


D = 3584
FF = 2560
WAVE = 2
MEMBERS = 8
GROUP_EP = 4
TOK_G = 512
CAP = 128
LANES = 128
EXTRA = 16


def as_sent(array):

    def short(part):
        return part.astype(jnp.bfloat16) if part.dtype == jnp.float32 else part

    return jax.tree.map(short, array)


def swapped(array, axis, distance):
    return lax.ppermute(array, axis, [(i, i ^ 1 << distance) for i in range(lax.axis_size(axis))])


def dispatch_slots(expert_ids, gate_values, live_count, expert):
    row_index = jnp.arange(TOK_G, dtype=jnp.int32)
    live_rows = row_index < live_count
    hit_mask = expert_ids == expert
    selected = jnp.logical_and(jnp.any(hit_mask, axis=1), live_rows)
    row_weight = jnp.sum(jnp.where(hit_mask, gate_values, jnp.float32(0.0)), axis=1)
    position = jnp.cumsum(selected.astype(jnp.int32)) - 1
    slot_index = jnp.arange(CAP, dtype=jnp.int32)
    slot_match = jnp.logical_and(position[None, :] == slot_index[:, None], selected[None, :])
    slot_rows = jnp.sum(jnp.where(slot_match, row_index[None, :], 0), axis=1)
    slot_valid = jnp.any(slot_match, axis=1)
    slot_weight = jnp.where(slot_valid, row_weight[slot_rows], jnp.float32(0.0))
    return (slot_rows, slot_weight)


def travelling(tokens, expert_ids, gate_values, group_counts, gate_weight, up_weight, down_weight):
    ep_index = lax.axis_index("ep")
    slice_width = FF // MEMBERS
    group_bits = GROUP_EP.bit_length() - 1
    weight_stack = jnp.stack([gate_weight, up_weight, down_weight])
    rows_held = weight_stack.shape[1]
    pieces = weight_stack.shape[2] // slice_width
    slice_blocks = weight_stack.reshape(3, rows_held, pieces, slice_width).transpose(0, 2, 1, 3)
    fan_out = lax.axis_size("ep") // pieces
    outgoing = jnp.tile(slice_blocks, (1, fan_out, 1, 1))
    arrived = lax.all_to_all(outgoing, "ep", split_axis=1, concat_axis=1, tiled=True)
    columns = arrived.reshape(3, -1, slice_width)
    features = lax.all_gather(tokens, "tp", axis=1, tiled=True)
    group_data = (features, expert_ids, gate_values)
    for bit_level in range(group_bits):
        received = jax.tree.map(
            lambda part, own: part.astype(own.dtype),
            swapped(as_sent(group_data), "ep", bit_level),
            group_data,
        )
        upper_half = ep_index >> bit_level & 1 == 1
        group_data = tuple(
            (
                jnp.where(
                    upper_half, jnp.concatenate([other, own], 0), jnp.concatenate([own, other], 0)
                )
                for own, other in zip(group_data, received)
            )
        )
    group_tokens, group_ids, group_gates = group_data
    live_count = lax.dynamic_index_in_dim(group_counts, ep_index // GROUP_EP, keepdims=False)
    partials = jnp.zeros((group_tokens.shape[0], D), jnp.float32)
    for expert in range(WAVE):
        slot_rows, slot_weight = dispatch_slots(group_ids, group_gates, live_count, expert)
        expert_rows = group_tokens[slot_rows]
        gate_cols = columns[0, expert * D : (expert + 1) * D]
        up_cols = columns[1, expert * D : (expert + 1) * D]
        down_cols = columns[2, expert * D : (expert + 1) * D]
        gate_act = jnp.dot(expert_rows, gate_cols, preferred_element_type=jnp.float32)
        up_act = jnp.dot(expert_rows, up_cols, preferred_element_type=jnp.float32)
        hidden = (jax.nn.silu(gate_act) * up_act).astype(jnp.bfloat16)
        projected = lax.dot_general(
            hidden, down_cols, (((1,), (1,)), ((), ())), preferred_element_type=jnp.float32
        )
        partials = partials.at[slot_rows].add(slot_weight[:, None] * projected)
    rounded = lax.optimization_barrier(partials.astype(jnp.bfloat16)).astype(jnp.float32)
    halved = lax.psum_scatter(
        rounded.astype(jnp.bfloat16), "tp", scatter_dimension=1, tiled=True
    ).astype(jnp.float32)
    for bit_level in reversed(range(group_bits)):
        paired_up = halved.reshape(2, -1, halved.shape[1])
        upper_half = ep_index >> bit_level & 1 == 1
        kept_part = jnp.where(upper_half, paired_up[1], paired_up[0])
        sent_part = jnp.where(upper_half, paired_up[0], paired_up[1])
        halved = kept_part + swapped(sent_part.astype(jnp.bfloat16), "ep", bit_level).astype(
            sent_part.dtype
        )
    return halved.astype(jnp.bfloat16)


def place_of(members):
    ep = lax.axis_index("ep")
    return ep // members, ep % members, lax.axis_index("tp")


def is_side(own_side, members):
    square, _, core = place_of(members)
    return (square == core) == own_side


def piece_copy(half, turn, members, destination, sem):
    _, member, core = place_of(members)
    width = destination.shape[1]
    per_half = half.shape[1] // width
    block = jnp.bitwise_xor(member, turn)
    columns = pl.ds(pl.multiple_of(block % per_half * width, LANES), width)
    return block // per_half == core, pltpu.make_async_copy(half.at[:, columns], destination, sem)


def pack_held_kernel(members, named, held, *refs):
    outs, (table_ref, sem) = refs[:members], refs[members:]
    rows = held.shape[0]
    pieces = [
        piece_copy(held, turn, members, out.at[:rows], sem.at[0, turn])
        for turn, out in enumerate(outs)
    ]
    for is_held, copy in pieces:
        pl.when(is_held)(copy.start)
    rest = named[...]
    table_ref[...] = jnp.zeros(table_ref.shape, table_ref.dtype)
    for term in range(3):
        part = rest.astype(jnp.bfloat16)
        rest = rest - part.astype(jnp.float32)
        table_ref[:WAVE, term * rows : (term + 1) * rows] = part
    tables = [
        pltpu.make_async_copy(table_ref, out.at[rows:], sem.at[1, turn])
        for turn, out in enumerate(outs)
    ]
    for copy in tables:
        copy.start()
    for copy in tables:
        copy.wait()
    for is_held, copy in pieces:
        pl.when(is_held)(copy.wait)


def pack_came_kernel(members, came, *refs):
    outs, sem = refs[members : 2 * members], refs[2 * members]
    rows = came.shape[0]
    pieces = [
        piece_copy(came, turn, members, out.at[:rows], sem.at[turn])
        for turn, out in enumerate(outs)
    ]
    for is_held, copy in pieces:
        pl.when(jnp.logical_not(is_held))(copy.start)
    for is_held, copy in pieces:
        pl.when(jnp.logical_not(is_held))(copy.wait)


def hold_kernel(array_ref, out_ref, sem):
    copy = pltpu.make_async_copy(array_ref, out_ref, sem)
    copy.start()
    copy.wait()


def routing_of(block, first, live, rows):
    extra = block[rows:, : 3 * LANES].astype(jnp.float32)
    weight = extra[:, :LANES] + extra[:, LANES : 2 * LANES] + extra[:, 2 * LANES :]
    return jnp.where(lax.broadcasted_iota(jnp.int32, weight.shape, 1) + first < live, weight, 0.0)


def compact_kernel(counts, *refs):
    blocks, (own_ref, other_ref, place_ref, weight_ref) = refs[:-4], refs[-4:]
    square, member, _ = place_of(len(blocks))
    slots = own_ref.shape[0]
    rows = blocks[0].shape[0] - EXTRA
    before = lax.broadcasted_iota(jnp.int32, (rows, rows), 0)
    after = lax.broadcasted_iota(jnp.int32, (rows, rows), 1)
    upto = (before <= after).astype(jnp.float32).astype(jnp.bfloat16)
    slot = lax.broadcasted_iota(jnp.int32, (slots, rows), 0)
    total = jnp.zeros((2 * slots, own_ref.shape[1]), jnp.float32)
    weights = [
        routing_of(block, jnp.bitwise_xor(member, turn) * rows, counts[square], rows)
        for turn, block in enumerate(blocks)
    ]
    counts = [
        jnp.dot(
            (weight > 0.0).astype(jnp.float32).astype(jnp.bfloat16),
            upto,
            preferred_element_type=jnp.float32,
        )
        for weight in weights
    ]
    for turn, block in enumerate(blocks):
        weight, count = weights[turn], counts[turn]
        for before, earlier in enumerate(counts):
            if before != turn:
                ahead = jnp.bitwise_xor(member, before) < jnp.bitwise_xor(member, turn)
                count = count + jnp.where(ahead, earlier[:, rows - 1 :], 0.0)
        place = jnp.where(weight > 0.0, count - 1.0, -1.0).astype(jnp.int32)
        pick = jnp.concatenate(
            [(slot == place[e : e + 1, :]).astype(jnp.float32) for e in range(WAVE)], 0
        ).astype(jnp.bfloat16)
        total = total + jnp.dot(pick, block[:rows, :], preferred_element_type=jnp.float32)
        place_ref[turn] = place[:8]
        weight_ref[turn] = weight[:8]
    own_ref[...] = total[:slots].astype(own_ref.dtype)
    other_ref[...] = total[slots:].astype(other_ref.dtype)


def spread_kernel(place_ref, weight_ref, _, pick_ref, column_ref):
    rows = place_ref.shape[2]
    slot = lax.broadcasted_iota(jnp.int32, (CAP, rows), 0)
    for turn in range(place_ref.shape[0]):
        place, weight = place_ref[turn], weight_ref[turn]
        for e in range(WAVE):
            pick = (slot == place[e : e + 1, :]).astype(jnp.float32)
            pick_ref[turn, :, e * CAP : (e + 1) * CAP] = pick.T.astype(pick_ref.dtype)
        table = jnp.where(slot == 0, weight[0:1, :], jnp.where(slot == 1, weight[1:2, :], 0.0))
        column_ref[turn] = table.T


def with_piece(members, turn, width, held, came, use):
    _, member, core = place_of(members)
    per_half = held[0].shape[1] // width
    block = jnp.bitwise_xor(member, turn)
    columns = pl.ds(pl.multiple_of(block % per_half * width, LANES), width)

    @pl.when(block // per_half == core)
    def _():
        use([half.at[:, columns] for half in held])

    @pl.when(block // per_half != core)
    def _():
        use([half.at[:, columns] for half in came])


def part_kernel(members, own_side, turn, rows_ref, *refs):
    held, came, out_ref = refs[:2], refs[2:4], refs[-1]
    width = out_ref.shape[1] // 2

    def use(weights):
        for n, weight in enumerate(weights):
            out_ref[:, n * width : (n + 1) * width] = jnp.dot(
                rows_ref[...], weight[...], preferred_element_type=jnp.float32
            ).astype(out_ref.dtype)

    @pl.when(is_side(own_side, members))
    def _():
        with_piece(members, turn, width, held, came, use)


def hidden_kernel(members, own_side, *refs):
    parts, out_ref = refs[:members], refs[-1]
    width = out_ref.shape[1]

    @pl.when(is_side(own_side, members))
    def _():
        gate, up = (
            sum(part[:, n * width : (n + 1) * width].astype(jnp.float32) for part in parts)
            for n in range(2)
        )
        out_ref[...] = (gate / (1.0 + jnp.exp(-gate)) * up).astype(out_ref.dtype)


def down_kernel(members, own_side, *refs):
    hidden, (held, came), (out_ref, total_ref) = refs[:members], refs[members : members + 2], refs[-2:]

    def use_turn(turn):
        def use(weights):
            product = lax.dot_general(
                hidden[turn][...],
                weights[0][...],
                (((1,), (1,)), ((), ())),
                preferred_element_type=jnp.float32,
            )
            total_ref[...] = product if turn == 0 else total_ref[...] + product

        return use

    @pl.when(is_side(own_side, members))
    def _():
        for turn in range(members):
            with_piece(members, turn, hidden[0].shape[1], [held], [came], use_turn(turn))
        out_ref[...] = total_ref[...].astype(out_ref.dtype)


def expand_kernel(own_ref, other_ref, pick_ref, column_ref, *outs):
    for turn, out in enumerate(outs):
        total = None
        for e, ref in enumerate((own_ref, other_ref)):
            chosen = jnp.dot(
                pick_ref[turn, :, e * CAP : (e + 1) * CAP],
                ref[...],
                preferred_element_type=jnp.float32,
            )
            part = column_ref[turn, :, e : e + 1] * chosen
            total = part if total is None else total + part
        out[...] = total.astype(out.dtype)


VMEM = pl.BlockSpec(memory_space=pltpu.VMEM)
SMEM = pl.BlockSpec(memory_space=pltpu.SMEM)
HBM = pl.BlockSpec(memory_space=pltpu.HBM)


def call(kernel, outs, specs, scratch=(), mib=8, space=VMEM, flops=0, aliases={}):
    return pl.pallas_call(
        kernel,
        out_shape=[jax.ShapeDtypeStruct(shape, dtype) for shape, dtype in outs],
        in_specs=specs,
        out_specs=[space] * len(outs),
        scratch_shapes=list(scratch),
        input_output_aliases=aliases,
        compiler_params=pltpu.CompilerParams(vmem_limit_bytes=mib * 1024 * 1024),
        cost_estimate=pl.CostEstimate(flops=flops, bytes_accessed=0, transcendentals=0),
    )


def moved(array, ep_size, tp_size, target):
    targets = {(e, t): target(e, t) for e in range(ep_size) for t in range(tp_size)}
    used = set(targets.values())
    pairs = []
    for (e, t), to in targets.items():
        if to is None:
            (to,) = [(e, core) for core in range(tp_size) if (e, core) not in used]
        pairs.append((e * tp_size + t, to[0] * tp_size + to[1]))
    return lax.ppermute(array, ("ep", "tp"), pairs)


def resting(
    tokens, expert_ids, gate_values, group_counts, gate_weight, up_weight, down_weight
):
    ep_size, tp_size = lax.axis_size("ep"), lax.axis_size("tp")
    ep, core = lax.axis_index("ep"), lax.axis_index("tp")
    rows = tokens.shape[0]
    members = TOK_G // rows
    per_core = members // tp_size
    member = ep % members
    thick = gate_weight.shape[0]
    width = tp_size * gate_weight.shape[1] // members
    bf16, f32 = jnp.bfloat16, jnp.float32
    send = functools.partial(moved, ep_size=ep_size, tp_size=tp_size)
    far_first = [members - 1 - n for n in range(members - 1)]

    def crosswise(turn, from_own):
        return lambda e, t: (
            (e ^ turn, tp_size - 1 - t) if (t == e // members) == from_own else None
        )

    def across(from_own):
        return lambda e, t: (
            ((e + members) % ep_size, t) if (t == e // members) == from_own else None
        )

    other_half = [(t, tp_size - 1 - t) for t in range(tp_size)]
    tokens_came = lax.ppermute(tokens, "tp", other_half)
    square = ep // members
    experts = jnp.stack([square, WAVE - 1 - square])[:, None, None]
    named = jnp.where(expert_ids.T[None] == experts, gate_values.T[None], 0.0).sum(1)
    blocks = [((rows + EXTRA, thick), bf16)] * members
    packed = call(
        functools.partial(pack_held_kernel, members),
        blocks,
        [VMEM, HBM],
        [pltpu.VMEM((EXTRA, thick), bf16), pltpu.SemaphoreType.DMA((2, members))],
        space=HBM,
    )(named, tokens)
    packed = call(
        functools.partial(pack_came_kernel, members),
        blocks,
        [HBM] * (1 + members),
        [pltpu.SemaphoreType.DMA((members,))],
        space=HBM,
        aliases={1 + turn: turn for turn in range(members)},
    )(tokens_came, *packed)
    arrived = {0: packed[0]}
    for turn in far_first:
        arrived[turn] = send(packed[turn], target=crosswise(turn, False))
    weights_came = []
    for weight in (gate_weight, up_weight, down_weight):
        weights_came.append(lax.ppermute(weight, "tp", other_half))
    gate_came, up_came, down_came = weights_came
    (up_held,) = call(
        hold_kernel, [(up_weight.shape, bf16)], [HBM], [pltpu.SemaphoreType.DMA], space=HBM
    )(up_weight)

    own_rows, other_rows, place, weight = call(
        compact_kernel,
        [
            ((CAP, thick), bf16),
            ((CAP, thick), bf16),
            ((members, 8, rows), jnp.int32),
            ((members, 8, rows), f32),
        ],
        [SMEM] + [VMEM] * members,
    )(group_counts, *[arrived[turn] for turn in range(members)])
    came_rows = send(other_rows, target=across(True))

    def parts_of(own_side, slot_rows, after):
        parts, last = {}, list(after)
        for turn in far_first + [0]:
            parts[turn] = call(
                functools.partial(part_kernel, members, own_side, turn),
                [((CAP, 2 * width), bf16)],
                [VMEM] * 5 + [HBM] * len(last),
                mib=16,
                flops=4 * CAP * thick * width,
            )(slot_rows, gate_weight, up_held, gate_came, up_came, *last)[0]
            last = [parts[turn]]
        came = []
        for turn in far_first + [0]:
            came.append(send(parts[turn], target=crosswise(turn, own_side)))
        return came, parts[0]

    def hidden_of(own_side, parts, after):
        hidden = call(
            functools.partial(hidden_kernel, members, not own_side),
            [((CAP, width), bf16)],
            [VMEM] * members + [HBM],
        )(*parts, after)[0]
        came = {}
        for turn in far_first + [0]:
            came[turn] = send(hidden, target=crosswise(turn, not own_side))
        return [came[turn] for turn in range(members)], hidden

    own_parts, own_last = parts_of(True, own_rows, [])
    other_parts, other_last = parts_of(False, came_rows, [own_last])
    own_hidden, own_last = hidden_of(True, own_parts, other_last)
    other_hidden, other_last = hidden_of(False, other_parts, own_last)

    def down_of(own_side, hidden, after):
        return call(
            functools.partial(down_kernel, members, own_side),
            [((CAP, thick), bf16)],
            [VMEM] * (members + 2) + [HBM],
            [pltpu.VMEM((CAP, thick), f32)],
            16,
        )(*hidden, down_weight, down_came, after)[0]

    own_projected = down_of(True, own_hidden, other_last)
    other_projected = down_of(False, other_hidden, own_projected)
    came_projected = send(other_projected, target=across(False))

    pick, column = call(
        spread_kernel,
        [((members, rows, WAVE * CAP), bf16), ((members, rows, LANES), f32)],
        [VMEM] * 2 + [HBM],
    )(place, weight, own_last)
    spread = call(
        expand_kernel, [((rows, thick), bf16)] * members, [VMEM] * 4
    )(own_projected, came_projected, pick, column)

    def back(turn):
        def target(e, t):
            return (e ^ turn, e % members // per_core) if e // members == t else None

        return target

    returned = {}
    for turn in far_first + [0]:
        returned[turn] = send(spread[turn], target=back(turn))
    low = core == member // per_core
    even, odd = (jnp.where(low, returned[n], returned[n + per_core]) for n in range(per_core))
    swap = member % per_core == 1
    return jnp.concatenate([jnp.where(swap, odd, even), jnp.where(swap, even, odd)], axis=1)


def shards(tokens, expert_ids, gate_values, group_counts, gate_weight, up_weight, down_weight):
    ep_size, tp_size = lax.axis_size("ep"), lax.axis_size("tp")
    members = TOK_G // tokens.shape[0]
    rests = ep_size == WAVE * members and tp_size == WAVE and members == 2 * tp_size
    return (resting if rests else travelling)(
        tokens, expert_ids, gate_values, group_counts, gate_weight, up_weight, down_weight
    )


def solution(mesh):
    placed = (
        P(("rep", "ep"), "tp"),
        P(("rep", "ep"), None),
        P(("rep", "ep"), None),
        P("rep"),
        P(("rep", "ep"), "tp"),
        P(("rep", "ep"), "tp"),
        P(("rep", "ep"), "tp"),
    )
    return jax.shard_map(
        shards, mesh=mesh, in_specs=placed, out_specs=P(("rep", "ep"), "tp"), check_vma=False
    )
```

```python
import functools

import jax
import jax.numpy as jnp
from jax import lax
from jax.experimental import pallas as pl
from jax.experimental.pallas import tpu as pltpu
from jax.sharding import PartitionSpec as P


D = 3584
FF = 2560
WAVE = 2
MEMBERS = 8
GROUP_EP = 4
TOK_G = 512
CAP = 128
LANES = 128
EXTRA = 8


def as_sent(array):

    def short(part):
        return part.astype(jnp.bfloat16) if part.dtype == jnp.float32 else part

    return jax.tree.map(short, array)


def swapped(array, axis, distance):
    return lax.ppermute(array, axis, [(i, i ^ 1 << distance) for i in range(lax.axis_size(axis))])


def dispatch_slots(expert_ids, gate_values, live_count, expert):
    row_index = jnp.arange(TOK_G, dtype=jnp.int32)
    live_rows = row_index < live_count
    hit_mask = expert_ids == expert
    selected = jnp.logical_and(jnp.any(hit_mask, axis=1), live_rows)
    row_weight = jnp.sum(jnp.where(hit_mask, gate_values, jnp.float32(0.0)), axis=1)
    position = jnp.cumsum(selected.astype(jnp.int32)) - 1
    slot_index = jnp.arange(CAP, dtype=jnp.int32)
    slot_match = jnp.logical_and(position[None, :] == slot_index[:, None], selected[None, :])
    slot_rows = jnp.sum(jnp.where(slot_match, row_index[None, :], 0), axis=1)
    slot_valid = jnp.any(slot_match, axis=1)
    slot_weight = jnp.where(slot_valid, row_weight[slot_rows], jnp.float32(0.0))
    return (slot_rows, slot_weight)


def travelling(tokens, expert_ids, gate_values, group_counts, gate_weight, up_weight, down_weight):
    ep_index = lax.axis_index("ep")
    slice_width = FF // MEMBERS
    group_bits = GROUP_EP.bit_length() - 1
    weight_stack = jnp.stack([gate_weight, up_weight, down_weight])
    rows_held = weight_stack.shape[1]
    pieces = weight_stack.shape[2] // slice_width
    slice_blocks = weight_stack.reshape(3, rows_held, pieces, slice_width).transpose(0, 2, 1, 3)
    fan_out = lax.axis_size("ep") // pieces
    outgoing = jnp.tile(slice_blocks, (1, fan_out, 1, 1))
    arrived = lax.all_to_all(outgoing, "ep", split_axis=1, concat_axis=1, tiled=True)
    columns = arrived.reshape(3, -1, slice_width)
    features = lax.all_gather(tokens, "tp", axis=1, tiled=True)
    group_data = (features, expert_ids, gate_values)
    for bit_level in range(group_bits):
        received = jax.tree.map(
            lambda part, own: part.astype(own.dtype),
            swapped(as_sent(group_data), "ep", bit_level),
            group_data,
        )
        upper_half = ep_index >> bit_level & 1 == 1
        group_data = tuple(
            (
                jnp.where(
                    upper_half, jnp.concatenate([other, own], 0), jnp.concatenate([own, other], 0)
                )
                for own, other in zip(group_data, received)
            )
        )
    group_tokens, group_ids, group_gates = group_data
    live_count = lax.dynamic_index_in_dim(group_counts, ep_index // GROUP_EP, keepdims=False)
    partials = jnp.zeros((group_tokens.shape[0], D), jnp.float32)
    for expert in range(WAVE):
        slot_rows, slot_weight = dispatch_slots(group_ids, group_gates, live_count, expert)
        expert_rows = group_tokens[slot_rows]
        gate_cols = columns[0, expert * D : (expert + 1) * D]
        up_cols = columns[1, expert * D : (expert + 1) * D]
        down_cols = columns[2, expert * D : (expert + 1) * D]
        gate_act = jnp.dot(expert_rows, gate_cols, preferred_element_type=jnp.float32)
        up_act = jnp.dot(expert_rows, up_cols, preferred_element_type=jnp.float32)
        hidden = (jax.nn.silu(gate_act) * up_act).astype(jnp.bfloat16)
        projected = lax.dot_general(
            hidden, down_cols, (((1,), (1,)), ((), ())), preferred_element_type=jnp.float32
        )
        partials = partials.at[slot_rows].add(slot_weight[:, None] * projected)
    rounded = lax.optimization_barrier(partials.astype(jnp.bfloat16)).astype(jnp.float32)
    halved = lax.psum_scatter(
        rounded.astype(jnp.bfloat16), "tp", scatter_dimension=1, tiled=True
    ).astype(jnp.float32)
    for bit_level in reversed(range(group_bits)):
        paired_up = halved.reshape(2, -1, halved.shape[1])
        upper_half = ep_index >> bit_level & 1 == 1
        kept_part = jnp.where(upper_half, paired_up[1], paired_up[0])
        sent_part = jnp.where(upper_half, paired_up[0], paired_up[1])
        halved = kept_part + swapped(sent_part.astype(jnp.bfloat16), "ep", bit_level).astype(
            sent_part.dtype
        )
    return halved.astype(jnp.bfloat16)


def place_of(members):
    ep = lax.axis_index("ep")
    return ep // members, ep % members, lax.axis_index("tp")


def is_side(own_side, members):
    square, _, core = place_of(members)
    return (square == core) == own_side


def piece_copy(half, turn, members, destination, sem):
    _, member, core = place_of(members)
    width = destination.shape[1]
    per_half = half.shape[1] // width
    block = jnp.bitwise_xor(member, turn)
    columns = pl.ds(pl.multiple_of(block % per_half * width, LANES), width)
    return block // per_half == core, pltpu.make_async_copy(half.at[:, columns], destination, sem)


def pack_held_kernel(members, named, held, *refs):
    outs, (table_ref, sem) = refs[:members], refs[members:]
    rows = held.shape[0]
    pieces = [
        piece_copy(held, turn, members, out.at[:rows], sem.at[0, turn])
        for turn, out in enumerate(outs)
    ]
    for is_held, copy in pieces:
        pl.when(is_held)(copy.start)
    rest = named[...]
    table_ref[...] = jnp.zeros(table_ref.shape, table_ref.dtype)
    for term in range(3):
        part = rest.astype(jnp.bfloat16)
        rest = rest - part.astype(jnp.float32)
        table_ref[:WAVE, term * rows : (term + 1) * rows] = part
    tables = [
        pltpu.make_async_copy(table_ref, out.at[rows:], sem.at[1, turn])
        for turn, out in enumerate(outs)
    ]
    for copy in tables:
        copy.start()
    for copy in tables:
        copy.wait()
    for is_held, copy in pieces:
        pl.when(is_held)(copy.wait)


def pack_came_kernel(members, came, *refs):
    outs, sem = refs[members : 2 * members], refs[2 * members]
    rows = came.shape[0]
    pieces = [
        piece_copy(came, turn, members, out.at[:rows], sem.at[turn])
        for turn, out in enumerate(outs)
    ]
    for is_held, copy in pieces:
        pl.when(jnp.logical_not(is_held))(copy.start)
    for is_held, copy in pieces:
        pl.when(jnp.logical_not(is_held))(copy.wait)


def hold_kernel(members, counts, array_ref, out_ref, live_ref, sem):
    copy = pltpu.make_async_copy(array_ref, out_ref, sem)
    copy.start()
    live_ref[...] = jnp.full(live_ref.shape, counts[place_of(members)[0]], live_ref.dtype)
    copy.wait()


def routing_of(block, first, live, rows):
    extra = block[rows:, : 3 * LANES].astype(jnp.float32)
    weight = extra[:, :LANES] + extra[:, LANES : 2 * LANES] + extra[:, 2 * LANES :]
    return jnp.where(lax.broadcasted_iota(jnp.int32, weight.shape, 1) + first < live, weight, 0.0)


def compact_kernel(live_ref, *refs):
    blocks, (own_ref, other_ref, routing_ref) = refs[:-3], refs[-3:]
    member = place_of(len(blocks))[1]
    slots = own_ref.shape[0]
    rows = blocks[0].shape[0] - EXTRA
    before = lax.broadcasted_iota(jnp.int32, (rows, rows), 0)
    after = lax.broadcasted_iota(jnp.int32, (rows, rows), 1)
    upto = (before <= after).astype(jnp.float32).astype(jnp.bfloat16)
    slot = lax.broadcasted_iota(jnp.int32, (slots, rows), 0)
    total = jnp.zeros((2 * slots, own_ref.shape[1]), jnp.float32)
    weights = [
        routing_of(block, jnp.bitwise_xor(member, turn) * rows, live_ref[:1, :], rows)
        for turn, block in enumerate(blocks)
    ]
    counts = [
        jnp.dot(
            (weight > 0.0).astype(jnp.float32).astype(jnp.bfloat16),
            upto,
            preferred_element_type=jnp.float32,
        )
        for weight in weights
    ]
    for turn, block in enumerate(blocks):
        weight, count = weights[turn], counts[turn]
        for before, earlier in enumerate(counts):
            if before != turn:
                ahead = jnp.bitwise_xor(member, before) < jnp.bitwise_xor(member, turn)
                count = count + jnp.where(ahead, earlier[:, rows - 1 :], 0.0)
        place = jnp.where(weight > 0.0, count - 1.0, -1.0).astype(jnp.int32)
        pick = jnp.concatenate(
            [(slot == place[e : e + 1, :]).astype(jnp.float32) for e in range(WAVE)], 0
        ).astype(jnp.bfloat16)
        total = total + jnp.dot(pick, block[:rows, :], preferred_element_type=jnp.float32)
        routing_ref[turn, :WAVE, :] = weight[:WAVE]
        routing_ref[turn, WAVE : 2 * WAVE, :] = place[:WAVE].astype(jnp.float32)
    own_ref[...] = total[:slots].astype(own_ref.dtype)
    other_ref[...] = total[slots:].astype(other_ref.dtype)


def spread_kernel(members, held_ref, came_ref, _, pick_ref, column_ref):
    square, _, core = place_of(members)
    rows = held_ref.shape[2]
    slot = lax.broadcasted_iota(jnp.int32, (CAP, rows), 0)
    for turn in range(members):
        routing = jnp.where(square == core, held_ref[turn], came_ref[turn])
        for e in range(WAVE):
            place = routing[WAVE + e : WAVE + e + 1, :].astype(jnp.int32)
            pick_ref[turn, :, e * CAP : (e + 1) * CAP] = (
                (slot == place).astype(jnp.float32).T.astype(pick_ref.dtype)
            )
        table = jnp.where(slot == 0, routing[0:1, :], jnp.where(slot == 1, routing[1:2, :], 0.0))
        column_ref[turn] = table.T


def with_piece(members, turn, width, held, came, use):
    _, member, core = place_of(members)
    per_half = held[0].shape[1] // width
    block = jnp.bitwise_xor(member, turn)
    columns = pl.ds(pl.multiple_of(block % per_half * width, LANES), width)

    @pl.when(block // per_half == core)
    def _():
        use([half.at[:, columns] for half in held])

    @pl.when(block // per_half != core)
    def _():
        use([half.at[:, columns] for half in came])


def part_kernel(members, own_side, turn, rows_ref, *refs):
    held, came, out_ref = refs[:2], refs[2:4], refs[-1]
    width = out_ref.shape[1] // 2

    def use(weights):
        for n, weight in enumerate(weights):
            out_ref[:, n * width : (n + 1) * width] = jnp.dot(
                rows_ref[...], weight[...], preferred_element_type=jnp.float32
            ).astype(out_ref.dtype)

    @pl.when(is_side(own_side, members))
    def _():
        with_piece(members, turn, width, held, came, use)


def hidden_kernel(members, own_side, *refs):
    parts, out_ref = refs[:members], refs[-1]
    width = out_ref.shape[1]

    @pl.when(is_side(own_side, members))
    def _():
        gate, up = (
            sum(part[:, n * width : (n + 1) * width].astype(jnp.float32) for part in parts)
            for n in range(2)
        )
        out_ref[...] = (gate / (1.0 + jnp.exp(-gate)) * up).astype(out_ref.dtype)


def down_kernel(members, own_side, turns, *refs):
    count = len(turns)
    hidden, (held, came), out_ref = refs[:count], refs[count : count + 2], refs[-2]
    earlier, total_ref = refs[count + 2], refs[-1]
    is_last = earlier.dtype == total_ref.dtype

    def use_turn(rows, is_first):
        def use(weights):
            product = lax.dot_general(
                rows[...],
                weights[0][...],
                (((1,), (1,)), ((), ())),
                preferred_element_type=jnp.float32,
            )
            total_ref[...] = product if is_first else total_ref[...] + product

        return use

    @pl.when(is_side(own_side, members))
    def _():
        if is_last:
            total_ref[...] = earlier[...]
        for n, turn in enumerate(turns):
            use = use_turn(hidden[n], n == 0 and not is_last)
            with_piece(members, turn, hidden[n].shape[1], [held], [came], use)
        out_ref[...] = total_ref[...].astype(out_ref.dtype)


def expand_kernel(turns, members, held_ref, came_ref, other_ref, pick_ref, column_ref, *outs):
    square, _, core = place_of(members)
    own = jnp.where(square == core, held_ref[...], came_ref[...])
    for turn, out in zip(turns, outs):
        total = None
        for e, slots in enumerate((own, other_ref[...])):
            chosen = jnp.dot(
                pick_ref[turn, :, e * CAP : (e + 1) * CAP],
                slots,
                preferred_element_type=jnp.float32,
            )
            part = column_ref[turn, :, e : e + 1] * chosen
            total = part if total is None else total + part
        out[...] = total.astype(out.dtype)


VMEM = pl.BlockSpec(memory_space=pltpu.VMEM)
SMEM = pl.BlockSpec(memory_space=pltpu.SMEM)
HBM = pl.BlockSpec(memory_space=pltpu.HBM)


def call(kernel, outs, specs, scratch=(), mib=8, space=VMEM, flops=0, aliases={}):
    return pl.pallas_call(
        kernel,
        out_shape=[jax.ShapeDtypeStruct(shape, dtype) for shape, dtype in outs],
        in_specs=specs,
        out_specs=space if isinstance(space, list) else [space] * len(outs),
        scratch_shapes=list(scratch),
        input_output_aliases=aliases,
        compiler_params=pltpu.CompilerParams(vmem_limit_bytes=mib * 1024 * 1024),
        cost_estimate=pl.CostEstimate(flops=flops, bytes_accessed=0, transcendentals=0),
    )


def moved(array, ep_size, tp_size, target):
    targets = {(e, t): target(e, t) for e in range(ep_size) for t in range(tp_size)}
    used = set(targets.values())
    pairs = []
    for (e, t), to in targets.items():
        if to is None:
            (free,) = [core for core in range(tp_size) if (e, core) not in used]
            to = (e, free) if free != t else (e ^ 1, t)
        pairs.append((e * tp_size + t, to[0] * tp_size + to[1]))
    return lax.ppermute(array, ("ep", "tp"), pairs)


def resting(
    tokens, expert_ids, gate_values, group_counts, gate_weight, up_weight, down_weight
):
    ep_size, tp_size = lax.axis_size("ep"), lax.axis_size("tp")
    ep, core = lax.axis_index("ep"), lax.axis_index("tp")
    rows = tokens.shape[0]
    members = TOK_G // rows
    per_core = members // tp_size
    member = ep % members
    thick = gate_weight.shape[0]
    width = tp_size * gate_weight.shape[1] // members
    bf16, f32 = jnp.bfloat16, jnp.float32
    send = functools.partial(moved, ep_size=ep_size, tp_size=tp_size)
    far_first = [members - 1 - n for n in range(members - 1)]

    def crosswise(turn, from_own):
        return lambda e, t: (
            (e ^ turn, tp_size - 1 - t) if (t == e // members) == from_own else None
        )

    def across(from_own):
        return lambda e, t: (
            ((e + members) % ep_size, t) if (t == e // members) == from_own else None
        )

    other_half = [(t, tp_size - 1 - t) for t in range(tp_size)]
    tokens_came = lax.ppermute(tokens, "tp", other_half)
    square = ep // members
    experts = jnp.stack([square, WAVE - 1 - square])[:, None, None]
    named = jnp.where(expert_ids.T[None] == experts, gate_values.T[None], 0.0).sum(1)
    blocks = [((rows + EXTRA, thick), bf16)] * members
    packed = call(
        functools.partial(pack_held_kernel, members),
        blocks,
        [VMEM, HBM],
        [pltpu.VMEM((EXTRA, thick), bf16), pltpu.SemaphoreType.DMA((2, members))],
        space=HBM,
    )(named, tokens)
    packed = call(
        functools.partial(pack_came_kernel, members),
        blocks,
        [HBM] * (1 + members),
        [pltpu.SemaphoreType.DMA((members,))],
        space=HBM,
        aliases={1 + turn: turn for turn in range(members)},
    )(tokens_came, *packed)
    arrived = {0: packed[0]}
    for turn in far_first:
        arrived[turn] = send(packed[turn], target=crosswise(turn, False))
    weights_came = []
    for weight in (gate_weight, up_weight, down_weight):
        weights_came.append(lax.ppermute(weight, "tp", other_half))
    gate_came, up_came, down_came = weights_came
    up_held, live = call(
        functools.partial(hold_kernel, members),
        [(up_weight.shape, bf16), ((8, rows), jnp.int32)],
        [SMEM, HBM],
        [pltpu.SemaphoreType.DMA],
        space=[HBM, VMEM],
    )(group_counts, up_weight)

    own_rows, other_rows, routing = call(
        compact_kernel,
        [
            ((CAP, thick), bf16),
            ((CAP, thick), bf16),
            ((members, 8, rows), f32),
        ],
        [VMEM] * (1 + members),
    )(live, *[arrived[turn] for turn in range(members)])
    came_rows = send(other_rows, target=across(True))

    def parts_of(own_side, slot_rows, after):
        parts, last = {}, list(after)
        for turn in far_first + [0]:
            parts[turn] = call(
                functools.partial(part_kernel, members, own_side, turn),
                [((CAP, 2 * width), bf16)],
                [VMEM] * 5 + [HBM] * len(last),
                mib=16,
                flops=4 * CAP * thick * width,
            )(slot_rows, gate_weight, up_held, gate_came, up_came, *last)[0]
            last = [parts[turn]]
        came = []
        for turn in far_first + [0]:
            came.append(send(parts[turn], target=crosswise(turn, own_side)))
        return came, parts[0]

    def hidden_of(own_side, parts, after):
        hidden = call(
            functools.partial(hidden_kernel, members, not own_side),
            [((CAP, width), bf16)],
            [VMEM] * members + [HBM],
        )(*parts, after)[0]
        came = {}
        for turn in far_first + [0]:
            came[turn] = send(hidden, target=crosswise(turn, not own_side))
        return [came[turn] for turn in range(members)], hidden

    own_parts, own_last = parts_of(True, own_rows, [])
    other_parts, other_last = parts_of(False, came_rows, [own_last])
    own_hidden, own_last = hidden_of(True, own_parts, other_last)
    other_hidden, other_last = hidden_of(False, other_parts, own_last)

    def down_of(own_side, hidden, after):
        total = after
        for turns, dtype in (((3, 2), f32), ((1, 0), bf16)):
            (total,) = call(
                functools.partial(down_kernel, members, own_side, turns),
                [((CAP, thick), dtype)],
                [VMEM] * (len(turns) + 2) + [VMEM],
                [pltpu.VMEM((CAP, thick), f32)],
                16,
            )(*[hidden[turn] for turn in turns], down_weight, down_came, total)
        return total

    own_projected = down_of(True, own_hidden, other_last)
    other_projected = down_of(False, other_hidden, own_projected)

    def to_leaver(e, t):
        return ((e + members) % ep_size, e % members // per_core) if t != e // members else None

    came_projected = send(other_projected, target=to_leaver)
    routing_came = lax.ppermute(routing, "tp", other_half)
    projected_came = lax.ppermute(own_projected, "tp", other_half)
    pick, column = call(
        functools.partial(spread_kernel, members),
        [((members, rows, WAVE * CAP), bf16), ((members, rows, LANES), f32)],
        [VMEM] * 2 + [HBM],
    )(routing, routing_came, own_last)

    def rows_of(*turns):
        return call(
            functools.partial(expand_kernel, turns, members),
            [((rows, thick), bf16)] * len(turns),
            [VMEM] * 5,
        )(own_projected, projected_came, came_projected, pick, column)

    near, far = rows_of(1, 3)
    kept, middle = rows_of(0, 2)

    def back(turn):
        def target(e, t):
            core = e % members // per_core
            return (e ^ turn, core) if (t == core) == (turn > 1) else None

        return target

    near = lax.ppermute(near, "tp", other_half)
    returned = {}
    for turn, block in ((3, far), (2, middle), (1, near)):
        returned[turn] = send(block, target=back(turn))
    here = core == member // per_core
    same = jnp.where(here, kept, returned[2])
    other = jnp.where(here, returned[1], returned[3])
    swap = member % per_core == 1
    return jnp.concatenate([jnp.where(swap, other, same), jnp.where(swap, same, other)], axis=1)


def shards(tokens, expert_ids, gate_values, group_counts, gate_weight, up_weight, down_weight):
    ep_size, tp_size = lax.axis_size("ep"), lax.axis_size("tp")
    members = TOK_G // tokens.shape[0]
    rests = ep_size == WAVE * members and tp_size == WAVE and members == 2 * tp_size
    return (resting if rests else travelling)(
        tokens, expert_ids, gate_values, group_counts, gate_weight, up_weight, down_weight
    )


def solution(mesh):
    placed = (
        P(("rep", "ep"), "tp"),
        P(("rep", "ep"), None),
        P(("rep", "ep"), None),
        P("rep"),
        P(("rep", "ep"), "tp"),
        P(("rep", "ep"), "tp"),
        P(("rep", "ep"), "tp"),
    )
    return jax.shard_map(
        shards, mesh=mesh, in_specs=placed, out_specs=P(("rep", "ep"), "tp"), check_vma=False
    )
```

```python
import functools

import jax
import jax.numpy as jnp
from jax import lax
from jax.experimental import pallas as pl
from jax.experimental.pallas import tpu as pltpu
from jax.sharding import PartitionSpec as P


D = 3584
FF = 2560
WAVE = 2
MEMBERS = 8
GROUP_EP = 4
TOK_G = 512
CAP = 128
LANES = 128
EXTRA = 8


def as_sent(array):

    def short(part):
        return part.astype(jnp.bfloat16) if part.dtype == jnp.float32 else part

    return jax.tree.map(short, array)


def swapped(array, axis, distance):
    return lax.ppermute(array, axis, [(i, i ^ 1 << distance) for i in range(lax.axis_size(axis))])


def dispatch_slots(expert_ids, gate_values, live_count, expert):
    row_index = jnp.arange(TOK_G, dtype=jnp.int32)
    live_rows = row_index < live_count
    hit_mask = expert_ids == expert
    selected = jnp.logical_and(jnp.any(hit_mask, axis=1), live_rows)
    row_weight = jnp.sum(jnp.where(hit_mask, gate_values, jnp.float32(0.0)), axis=1)
    position = jnp.cumsum(selected.astype(jnp.int32)) - 1
    slot_index = jnp.arange(CAP, dtype=jnp.int32)
    slot_match = jnp.logical_and(position[None, :] == slot_index[:, None], selected[None, :])
    slot_rows = jnp.sum(jnp.where(slot_match, row_index[None, :], 0), axis=1)
    slot_valid = jnp.any(slot_match, axis=1)
    slot_weight = jnp.where(slot_valid, row_weight[slot_rows], jnp.float32(0.0))
    return (slot_rows, slot_weight)


def travelling(tokens, expert_ids, gate_values, group_counts, gate_weight, up_weight, down_weight):
    ep_index = lax.axis_index("ep")
    slice_width = FF // MEMBERS
    group_bits = GROUP_EP.bit_length() - 1
    weight_stack = jnp.stack([gate_weight, up_weight, down_weight])
    rows_held = weight_stack.shape[1]
    pieces = weight_stack.shape[2] // slice_width
    slice_blocks = weight_stack.reshape(3, rows_held, pieces, slice_width).transpose(0, 2, 1, 3)
    fan_out = lax.axis_size("ep") // pieces
    outgoing = jnp.tile(slice_blocks, (1, fan_out, 1, 1))
    arrived = lax.all_to_all(outgoing, "ep", split_axis=1, concat_axis=1, tiled=True)
    columns = arrived.reshape(3, -1, slice_width)
    features = lax.all_gather(tokens, "tp", axis=1, tiled=True)
    group_data = (features, expert_ids, gate_values)
    for bit_level in range(group_bits):
        received = jax.tree.map(
            lambda part, own: part.astype(own.dtype),
            swapped(as_sent(group_data), "ep", bit_level),
            group_data,
        )
        upper_half = ep_index >> bit_level & 1 == 1
        group_data = tuple(
            (
                jnp.where(
                    upper_half, jnp.concatenate([other, own], 0), jnp.concatenate([own, other], 0)
                )
                for own, other in zip(group_data, received)
            )
        )
    group_tokens, group_ids, group_gates = group_data
    live_count = lax.dynamic_index_in_dim(group_counts, ep_index // GROUP_EP, keepdims=False)
    partials = jnp.zeros((group_tokens.shape[0], D), jnp.float32)
    for expert in range(WAVE):
        slot_rows, slot_weight = dispatch_slots(group_ids, group_gates, live_count, expert)
        expert_rows = group_tokens[slot_rows]
        gate_cols = columns[0, expert * D : (expert + 1) * D]
        up_cols = columns[1, expert * D : (expert + 1) * D]
        down_cols = columns[2, expert * D : (expert + 1) * D]
        gate_act = jnp.dot(expert_rows, gate_cols, preferred_element_type=jnp.float32)
        up_act = jnp.dot(expert_rows, up_cols, preferred_element_type=jnp.float32)
        hidden = (jax.nn.silu(gate_act) * up_act).astype(jnp.bfloat16)
        projected = lax.dot_general(
            hidden, down_cols, (((1,), (1,)), ((), ())), preferred_element_type=jnp.float32
        )
        partials = partials.at[slot_rows].add(slot_weight[:, None] * projected)
    rounded = lax.optimization_barrier(partials.astype(jnp.bfloat16)).astype(jnp.float32)
    halved = lax.psum_scatter(
        rounded.astype(jnp.bfloat16), "tp", scatter_dimension=1, tiled=True
    ).astype(jnp.float32)
    for bit_level in reversed(range(group_bits)):
        paired_up = halved.reshape(2, -1, halved.shape[1])
        upper_half = ep_index >> bit_level & 1 == 1
        kept_part = jnp.where(upper_half, paired_up[1], paired_up[0])
        sent_part = jnp.where(upper_half, paired_up[0], paired_up[1])
        halved = kept_part + swapped(sent_part.astype(jnp.bfloat16), "ep", bit_level).astype(
            sent_part.dtype
        )
    return halved.astype(jnp.bfloat16)


def place_of(members):
    ep = lax.axis_index("ep")
    return ep // members, ep % members, lax.axis_index("tp")


def is_side(own_side, members):
    square, _, core = place_of(members)
    return (square == core) == own_side


def piece_copy(half, turn, members, destination, sem):
    _, member, core = place_of(members)
    width = destination.shape[1]
    per_half = half.shape[1] // width
    block = jnp.bitwise_xor(member, turn)
    columns = pl.ds(pl.multiple_of(block % per_half * width, LANES), width)
    return block // per_half == core, pltpu.make_async_copy(half.at[:, columns], destination, sem)


def pack_held_kernel(members, named, held, *refs):
    outs, (table_ref, sem) = refs[:members], refs[members:]
    rows = held.shape[0]
    pieces = [
        piece_copy(held, turn, members, out.at[:rows], sem.at[0, turn])
        for turn, out in enumerate(outs)
    ]
    for is_held, copy in pieces:
        pl.when(is_held)(copy.start)
    rest = named[...]
    table_ref[...] = jnp.zeros(table_ref.shape, table_ref.dtype)
    for term in range(3):
        part = rest.astype(jnp.bfloat16)
        rest = rest - part.astype(jnp.float32)
        table_ref[:WAVE, term * rows : (term + 1) * rows] = part
    tables = [
        pltpu.make_async_copy(table_ref, out.at[rows:], sem.at[1, turn])
        for turn, out in enumerate(outs)
    ]
    for copy in tables:
        copy.start()
    for copy in tables:
        copy.wait()
    for is_held, copy in pieces:
        pl.when(is_held)(copy.wait)


def pack_came_kernel(members, came, *refs):
    outs, sem = refs[members : 2 * members], refs[2 * members]
    rows = came.shape[0]
    pieces = [
        piece_copy(came, turn, members, out.at[:rows], sem.at[turn])
        for turn, out in enumerate(outs)
    ]
    for is_held, copy in pieces:
        pl.when(jnp.logical_not(is_held))(copy.start)
    for is_held, copy in pieces:
        pl.when(jnp.logical_not(is_held))(copy.wait)


def hold_kernel(members, counts, array_ref, out_ref, live_ref, sem):
    copy = pltpu.make_async_copy(array_ref, out_ref, sem)
    copy.start()
    live_ref[...] = jnp.full(live_ref.shape, counts[place_of(members)[0]], live_ref.dtype)
    copy.wait()


def routing_of(block, first, live, rows):
    extra = block[rows:, : 3 * LANES].astype(jnp.float32)
    weight = extra[:, :LANES] + extra[:, LANES : 2 * LANES] + extra[:, 2 * LANES :]
    return jnp.where(lax.broadcasted_iota(jnp.int32, weight.shape, 1) + first < live, weight, 0.0)


def compact_kernel(live_ref, *refs):
    blocks, (own_ref, other_ref, routing_ref) = refs[:-3], refs[-3:]
    member = place_of(len(blocks))[1]
    slots = own_ref.shape[0]
    rows = blocks[0].shape[0] - EXTRA
    before = lax.broadcasted_iota(jnp.int32, (rows, rows), 0)
    after = lax.broadcasted_iota(jnp.int32, (rows, rows), 1)
    upto = (before <= after).astype(jnp.float32).astype(jnp.bfloat16)
    slot = lax.broadcasted_iota(jnp.int32, (slots, rows), 0)
    total = jnp.zeros((2 * slots, own_ref.shape[1]), jnp.float32)
    weights = [
        routing_of(block, jnp.bitwise_xor(member, turn) * rows, live_ref[:1, :], rows)
        for turn, block in enumerate(blocks)
    ]
    counts = [
        jnp.dot(
            (weight > 0.0).astype(jnp.float32).astype(jnp.bfloat16),
            upto,
            preferred_element_type=jnp.float32,
        )
        for weight in weights
    ]
    for turn, block in enumerate(blocks):
        weight, count = weights[turn], counts[turn]
        for before, earlier in enumerate(counts):
            if before != turn:
                ahead = jnp.bitwise_xor(member, before) < jnp.bitwise_xor(member, turn)
                count = count + jnp.where(ahead, earlier[:, rows - 1 :], 0.0)
        place = jnp.where(weight > 0.0, count - 1.0, -1.0).astype(jnp.int32)
        pick = jnp.concatenate(
            [(slot == place[e : e + 1, :]).astype(jnp.float32) for e in range(WAVE)], 0
        ).astype(jnp.bfloat16)
        total = total + jnp.dot(pick, block[:rows, :], preferred_element_type=jnp.float32)
        routing_ref[turn, :WAVE, :] = weight[:WAVE]
        routing_ref[turn, WAVE : 2 * WAVE, :] = place[:WAVE].astype(jnp.float32)
    own_ref[...] = total[:slots].astype(own_ref.dtype)
    other_ref[...] = total[slots:].astype(other_ref.dtype)


def spread_kernel(members, held_ref, came_ref, _, pick_ref, column_ref):
    square, _, core = place_of(members)
    rows = held_ref.shape[2]
    slot = lax.broadcasted_iota(jnp.int32, (CAP, rows), 0)
    for turn in range(members):
        routing = jnp.where(square == core, held_ref[turn], came_ref[turn])
        for e in range(WAVE):
            place = routing[WAVE + e : WAVE + e + 1, :].astype(jnp.int32)
            pick_ref[turn, :, e * CAP : (e + 1) * CAP] = (
                (slot == place).astype(jnp.float32).T.astype(pick_ref.dtype)
            )
        table = jnp.where(slot == 0, routing[0:1, :], jnp.where(slot == 1, routing[1:2, :], 0.0))
        column_ref[turn] = table.T


def with_piece(members, turn, width, held, came, use):
    _, member, core = place_of(members)
    per_half = held[0].shape[1] // width
    block = jnp.bitwise_xor(member, turn)
    columns = pl.ds(pl.multiple_of(block % per_half * width, LANES), width)

    @pl.when(block // per_half == core)
    def _():
        use([half.at[:, columns] for half in held])

    @pl.when(block // per_half != core)
    def _():
        use([half.at[:, columns] for half in came])


def part_kernel(members, own_side, turn, rows_ref, *refs):
    held, came, out_ref = refs[:2], refs[2:4], refs[-1]
    width = out_ref.shape[1] // 2

    def use(weights):
        for n, weight in enumerate(weights):
            out_ref[:, n * width : (n + 1) * width] = jnp.dot(
                rows_ref[...], weight[...], preferred_element_type=jnp.float32
            ).astype(out_ref.dtype)

    @pl.when(is_side(own_side, members))
    def _():
        with_piece(members, turn, width, held, came, use)


def hidden_kernel(members, own_side, *refs):
    parts, out_ref = refs[:members], refs[-1]
    width = out_ref.shape[1]

    @pl.when(is_side(own_side, members))
    def _():
        gate, up = (
            sum(part[:, n * width : (n + 1) * width].astype(jnp.float32) for part in parts)
            for n in range(2)
        )
        out_ref[...] = (gate / (1.0 + jnp.exp(-gate)) * up).astype(out_ref.dtype)


def down_kernel(members, own_side, turns, *refs):
    count = len(turns)
    hidden, (held, came), out_ref = refs[:count], refs[count : count + 2], refs[-2]
    earlier, total_ref = refs[count + 2], refs[-1]
    is_last = earlier.dtype == total_ref.dtype

    def use_turn(rows, is_first):
        def use(weights):
            product = lax.dot_general(
                rows[...],
                weights[0][...],
                (((1,), (1,)), ((), ())),
                preferred_element_type=jnp.float32,
            )
            total_ref[...] = product if is_first else total_ref[...] + product

        return use

    @pl.when(is_side(own_side, members))
    def _():
        if is_last:
            total_ref[...] = earlier[...]
        for n, turn in enumerate(turns):
            use = use_turn(hidden[n], n == 0 and not is_last)
            with_piece(members, turn, hidden[n].shape[1], [held], [came], use)
        out_ref[...] = total_ref[...].astype(out_ref.dtype)


def expand_kernel(turns, members, held_ref, came_ref, other_ref, pick_ref, column_ref, *outs):
    square, _, core = place_of(members)
    own = jnp.where(square == core, held_ref[...], came_ref[...])
    for turn, out in zip(turns, outs):
        total = None
        for e, slots in enumerate((own, other_ref[...])):
            chosen = jnp.dot(
                pick_ref[turn, :, e * CAP : (e + 1) * CAP],
                slots,
                preferred_element_type=jnp.float32,
            )
            part = column_ref[turn, :, e : e + 1] * chosen
            total = part if total is None else total + part
        out[...] = total.astype(out.dtype)


VMEM = pl.BlockSpec(memory_space=pltpu.VMEM)
SMEM = pl.BlockSpec(memory_space=pltpu.SMEM)
HBM = pl.BlockSpec(memory_space=pltpu.HBM)


def call(kernel, outs, specs, scratch=(), mib=8, space=VMEM, flops=0, aliases={}):
    return pl.pallas_call(
        kernel,
        out_shape=[jax.ShapeDtypeStruct(shape, dtype) for shape, dtype in outs],
        in_specs=specs,
        out_specs=space if isinstance(space, list) else [space] * len(outs),
        scratch_shapes=list(scratch),
        input_output_aliases=aliases,
        compiler_params=pltpu.CompilerParams(vmem_limit_bytes=mib * 1024 * 1024),
        cost_estimate=pl.CostEstimate(flops=flops, bytes_accessed=0, transcendentals=0),
    )


def moved(array, ep_size, tp_size, target):
    targets = {(e, t): target(e, t) for e in range(ep_size) for t in range(tp_size)}
    used = set(targets.values())
    pairs = []
    for (e, t), to in targets.items():
        if to is None:
            (free,) = [core for core in range(tp_size) if (e, core) not in used]
            to = (e, free) if free != t else (e ^ 1, t)
        pairs.append((e * tp_size + t, to[0] * tp_size + to[1]))
    return lax.ppermute(array, ("ep", "tp"), pairs)


def resting(
    tokens, expert_ids, gate_values, group_counts, gate_weight, up_weight, down_weight
):
    ep_size, tp_size = lax.axis_size("ep"), lax.axis_size("tp")
    ep, core = lax.axis_index("ep"), lax.axis_index("tp")
    rows = tokens.shape[0]
    members = TOK_G // rows
    per_core = members // tp_size
    member = ep % members
    thick = gate_weight.shape[0]
    width = tp_size * gate_weight.shape[1] // members
    bf16, f32 = jnp.bfloat16, jnp.float32
    send = functools.partial(moved, ep_size=ep_size, tp_size=tp_size)
    far_first = [members - 1 - n for n in range(members - 1)]

    def crosswise(turn, from_own):
        return lambda e, t: (
            (e ^ turn, tp_size - 1 - t) if (t == e // members) == from_own else None
        )

    def across(from_own):
        return lambda e, t: (
            ((e + members) % ep_size, t) if (t == e // members) == from_own else None
        )

    other_half = [(t, tp_size - 1 - t) for t in range(tp_size)]
    tokens_came = lax.ppermute(tokens, "tp", other_half)
    square = ep // members
    experts = jnp.stack([square, WAVE - 1 - square])[:, None, None]
    named = jnp.where(expert_ids.T[None] == experts, gate_values.T[None], 0.0).sum(1)
    blocks = [((rows + EXTRA, thick), bf16)] * members
    packed = call(
        functools.partial(pack_held_kernel, members),
        blocks,
        [VMEM, HBM],
        [pltpu.VMEM((EXTRA, thick), bf16), pltpu.SemaphoreType.DMA((2, members))],
        space=HBM,
    )(named, tokens)
    packed = call(
        functools.partial(pack_came_kernel, members),
        blocks,
        [HBM] * (1 + members),
        [pltpu.SemaphoreType.DMA((members,))],
        space=HBM,
        aliases={1 + turn: turn for turn in range(members)},
    )(tokens_came, *packed)
    arrived = {0: packed[0]}
    for turn in far_first:
        arrived[turn] = send(packed[turn], target=crosswise(turn, False))
    weights_came = []
    for weight in (gate_weight, up_weight, down_weight):
        weights_came.append(lax.ppermute(weight, "tp", other_half))
    gate_came, up_came, down_came = weights_came
    up_held, live = call(
        functools.partial(hold_kernel, members),
        [(up_weight.shape, bf16), ((8, rows), jnp.int32)],
        [SMEM, HBM],
        [pltpu.SemaphoreType.DMA],
        space=[HBM, VMEM],
    )(group_counts, up_weight)

    own_rows, other_rows, routing = call(
        compact_kernel,
        [
            ((CAP, thick), bf16),
            ((CAP, thick), bf16),
            ((members, 8, rows), f32),
        ],
        [VMEM] * (1 + members),
    )(live, *[arrived[turn] for turn in range(members)])
    came_rows = send(other_rows, target=across(True))

    def parts_of(own_side, slot_rows, after):
        parts, last = {}, list(after)
        for turn in far_first + [0]:
            parts[turn] = call(
                functools.partial(part_kernel, members, own_side, turn),
                [((CAP, 2 * width), bf16)],
                [VMEM] * 5 + [HBM] * len(last),
                mib=16,
                flops=4 * CAP * thick * width,
            )(slot_rows, gate_weight, up_held, gate_came, up_came, *last)[0]
            last = [parts[turn]]
        came = []
        for turn in far_first + [0]:
            came.append(send(parts[turn], target=crosswise(turn, own_side)))
        return came, parts[0]

    def hidden_of(own_side, parts, after):
        hidden = call(
            functools.partial(hidden_kernel, members, not own_side),
            [((CAP, width), bf16)],
            [VMEM] * members + [HBM],
        )(*parts, after)[0]
        came = {}
        for turn in far_first + [0]:
            came[turn] = send(hidden, target=crosswise(turn, not own_side))
        return came, hidden

    own_parts, own_last = parts_of(True, own_rows, [])
    other_parts, other_last = parts_of(False, came_rows, [own_last])
    own_hidden, own_last = hidden_of(True, own_parts, other_last)
    other_hidden, other_last = hidden_of(False, other_parts, own_last)

    def down_of(own_side, hidden, after):
        total = after
        for turns, dtype in (((3, 2), f32), ((1, 0), bf16)):
            (total,) = call(
                functools.partial(down_kernel, members, own_side, turns),
                [((CAP, thick), dtype)],
                [VMEM] * (len(turns) + 2) + [VMEM],
                [pltpu.VMEM((CAP, thick), f32)],
                16,
            )(*[hidden[turn] for turn in turns], down_weight, down_came, total)
        return total

    other_projected = down_of(False, other_hidden, other_last)
    own_projected = down_of(True, own_hidden, other_projected)

    def to_leaver(e, t):
        return ((e + members) % ep_size, e % members // per_core) if t != e // members else None

    came_projected = send(other_projected, target=to_leaver)
    routing_came = lax.ppermute(routing, "tp", other_half)
    projected_came = lax.ppermute(own_projected, "tp", other_half)
    pick, column = call(
        functools.partial(spread_kernel, members),
        [((members, rows, WAVE * CAP), bf16), ((members, rows, LANES), f32)],
        [VMEM] * 2 + [HBM],
    )(routing, routing_came, own_last)

    def rows_of(*turns):
        return call(
            functools.partial(expand_kernel, turns, members),
            [((rows, thick), bf16)] * len(turns),
            [VMEM] * 5,
        )(own_projected, projected_came, came_projected, pick, column)

    near, far = rows_of(1, 3)
    kept, middle = rows_of(0, 2)

    def back(turn):
        def target(e, t):
            core = e % members // per_core
            return (e ^ turn, core) if (t == core) == (turn > 1) else None

        return target

    near = lax.ppermute(near, "tp", other_half)
    returned = {}
    for turn, block in ((3, far), (2, middle), (1, near)):
        returned[turn] = send(block, target=back(turn))
    here = core == member // per_core
    same = jnp.where(here, kept, returned[2])
    other = jnp.where(here, returned[1], returned[3])
    swap = member % per_core == 1
    return jnp.concatenate([jnp.where(swap, other, same), jnp.where(swap, same, other)], axis=1)


def shards(tokens, expert_ids, gate_values, group_counts, gate_weight, up_weight, down_weight):
    ep_size, tp_size = lax.axis_size("ep"), lax.axis_size("tp")
    members = TOK_G // tokens.shape[0]
    rests = ep_size == WAVE * members and tp_size == WAVE and members == 2 * tp_size
    return (resting if rests else travelling)(
        tokens, expert_ids, gate_values, group_counts, gate_weight, up_weight, down_weight
    )


def solution(mesh):
    placed = (
        P(("rep", "ep"), "tp"),
        P(("rep", "ep"), None),
        P(("rep", "ep"), None),
        P("rep"),
        P(("rep", "ep"), "tp"),
        P(("rep", "ep"), "tp"),
        P(("rep", "ep"), "tp"),
    )
    return jax.shard_map(
        shards, mesh=mesh, in_specs=placed, out_specs=P(("rep", "ep"), "tp"), check_vma=False
    )
```

```python
import functools

import jax
import jax.numpy as jnp
from jax import lax
from jax.experimental import pallas as pl
from jax.experimental.pallas import tpu as pltpu
from jax.sharding import PartitionSpec as P


D = 3584
FF = 2560
WAVE = 2
MEMBERS = 8
GROUP_EP = 4
TOK_G = 512
CAP = 128
LANES = 128
EXTRA = 8


def as_sent(array):

    def short(part):
        return part.astype(jnp.bfloat16) if part.dtype == jnp.float32 else part

    return jax.tree.map(short, array)


def swapped(array, axis, distance):
    return lax.ppermute(array, axis, [(i, i ^ 1 << distance) for i in range(lax.axis_size(axis))])


def dispatch_slots(expert_ids, gate_values, live_count, expert):
    row_index = jnp.arange(TOK_G, dtype=jnp.int32)
    live_rows = row_index < live_count
    hit_mask = expert_ids == expert
    selected = jnp.logical_and(jnp.any(hit_mask, axis=1), live_rows)
    row_weight = jnp.sum(jnp.where(hit_mask, gate_values, jnp.float32(0.0)), axis=1)
    position = jnp.cumsum(selected.astype(jnp.int32)) - 1
    slot_index = jnp.arange(CAP, dtype=jnp.int32)
    slot_match = jnp.logical_and(position[None, :] == slot_index[:, None], selected[None, :])
    slot_rows = jnp.sum(jnp.where(slot_match, row_index[None, :], 0), axis=1)
    slot_valid = jnp.any(slot_match, axis=1)
    slot_weight = jnp.where(slot_valid, row_weight[slot_rows], jnp.float32(0.0))
    return (slot_rows, slot_weight)


def travelling(tokens, expert_ids, gate_values, group_counts, gate_weight, up_weight, down_weight):
    ep_index = lax.axis_index("ep")
    slice_width = FF // MEMBERS
    group_bits = GROUP_EP.bit_length() - 1
    weight_stack = jnp.stack([gate_weight, up_weight, down_weight])
    rows_held = weight_stack.shape[1]
    pieces = weight_stack.shape[2] // slice_width
    slice_blocks = weight_stack.reshape(3, rows_held, pieces, slice_width).transpose(0, 2, 1, 3)
    fan_out = lax.axis_size("ep") // pieces
    outgoing = jnp.tile(slice_blocks, (1, fan_out, 1, 1))
    arrived = lax.all_to_all(outgoing, "ep", split_axis=1, concat_axis=1, tiled=True)
    columns = arrived.reshape(3, -1, slice_width)
    features = lax.all_gather(tokens, "tp", axis=1, tiled=True)
    group_data = (features, expert_ids, gate_values)
    for bit_level in range(group_bits):
        received = jax.tree.map(
            lambda part, own: part.astype(own.dtype),
            swapped(as_sent(group_data), "ep", bit_level),
            group_data,
        )
        upper_half = ep_index >> bit_level & 1 == 1
        group_data = tuple(
            (
                jnp.where(
                    upper_half, jnp.concatenate([other, own], 0), jnp.concatenate([own, other], 0)
                )
                for own, other in zip(group_data, received)
            )
        )
    group_tokens, group_ids, group_gates = group_data
    live_count = lax.dynamic_index_in_dim(group_counts, ep_index // GROUP_EP, keepdims=False)
    partials = jnp.zeros((group_tokens.shape[0], D), jnp.float32)
    for expert in range(WAVE):
        slot_rows, slot_weight = dispatch_slots(group_ids, group_gates, live_count, expert)
        expert_rows = group_tokens[slot_rows]
        gate_cols = columns[0, expert * D : (expert + 1) * D]
        up_cols = columns[1, expert * D : (expert + 1) * D]
        down_cols = columns[2, expert * D : (expert + 1) * D]
        gate_act = jnp.dot(expert_rows, gate_cols, preferred_element_type=jnp.float32)
        up_act = jnp.dot(expert_rows, up_cols, preferred_element_type=jnp.float32)
        hidden = (jax.nn.silu(gate_act) * up_act).astype(jnp.bfloat16)
        projected = lax.dot_general(
            hidden, down_cols, (((1,), (1,)), ((), ())), preferred_element_type=jnp.float32
        )
        partials = partials.at[slot_rows].add(slot_weight[:, None] * projected)
    rounded = lax.optimization_barrier(partials.astype(jnp.bfloat16)).astype(jnp.float32)
    halved = lax.psum_scatter(
        rounded.astype(jnp.bfloat16), "tp", scatter_dimension=1, tiled=True
    ).astype(jnp.float32)
    for bit_level in reversed(range(group_bits)):
        paired_up = halved.reshape(2, -1, halved.shape[1])
        upper_half = ep_index >> bit_level & 1 == 1
        kept_part = jnp.where(upper_half, paired_up[1], paired_up[0])
        sent_part = jnp.where(upper_half, paired_up[0], paired_up[1])
        halved = kept_part + swapped(sent_part.astype(jnp.bfloat16), "ep", bit_level).astype(
            sent_part.dtype
        )
    return halved.astype(jnp.bfloat16)


def place_of(members):
    ep = lax.axis_index("ep")
    return ep // members, ep % members, lax.axis_index("tp")


def is_side(own_side, members):
    square, _, core = place_of(members)
    return (square == core) == own_side


def piece_copies(half, turn, members, parts, rows, sems):
    _, member, core = place_of(members)
    width = sum(part.shape[1] for part in parts)
    per_half = half.shape[1] // width
    block = jnp.bitwise_xor(member, turn)
    copies, first = [], block % per_half * width
    for n, part in enumerate(parts):
        columns = pl.ds(pl.multiple_of(first, LANES), part.shape[1])
        copies.append(pltpu.make_async_copy(half.at[:, columns], part.at[:rows], sems.at[n]))
        first = first + part.shape[1]
    return block // per_half == core, copies


def run_when(condition, copies):
    @pl.when(condition)
    def _():
        for copy in copies:
            copy()


def pack_held_kernel(members, named, held, *refs):
    outs, (table_ref, sem) = refs[: 2 * members], refs[2 * members :]
    rows = held.shape[0]
    pieces = [
        piece_copies(held, turn, members, outs[turn::members], rows, sem.at[turn])
        for turn in range(members)
    ]
    for is_held, copies in pieces:
        run_when(is_held, [copy.start for copy in copies])
    rest = named[...]
    table_ref[...] = jnp.zeros(table_ref.shape, table_ref.dtype)
    for term in range(3):
        part = rest.astype(jnp.bfloat16)
        rest = rest - part.astype(jnp.float32)
        table_ref[:WAVE, term * rows : (term + 1) * rows] = part
    tables = [
        pltpu.make_async_copy(table_ref, outs[turn].at[rows:], sem.at[turn, 2])
        for turn in range(members)
    ]
    for copy in tables:
        copy.start()
    for copy in tables:
        copy.wait()
    for is_held, copies in pieces:
        run_when(is_held, [copy.wait for copy in copies])


def pack_came_kernel(members, came, *refs):
    outs, sem = refs[2 * members : 4 * members], refs[4 * members]
    rows = came.shape[0]
    pieces = [
        piece_copies(came, turn, members, outs[turn::members], rows, sem.at[turn])
        for turn in range(members)
    ]
    for is_held, copies in pieces:
        run_when(jnp.logical_not(is_held), [copy.start for copy in copies])
    for is_held, copies in pieces:
        run_when(jnp.logical_not(is_held), [copy.wait for copy in copies])


def hold_kernel(members, counts, array_ref, out_ref, live_ref, sem):
    copy = pltpu.make_async_copy(array_ref, out_ref, sem)
    copy.start()
    live_ref[...] = jnp.full(live_ref.shape, counts[place_of(members)[0]], live_ref.dtype)
    copy.wait()


def routing_of(block, first, live, rows):
    extra = block[rows:, : 3 * LANES].astype(jnp.float32)
    weight = extra[:, :LANES] + extra[:, LANES : 2 * LANES] + extra[:, 2 * LANES :]
    return jnp.where(lax.broadcasted_iota(jnp.int32, weight.shape, 1) + first < live, weight, 0.0)


def compact_kernel(live_ref, *refs):
    blocks, (own_ref, other_ref, routing_ref) = refs[:-3], refs[-3:]
    member = place_of(len(blocks))[1]
    slots = own_ref.shape[0]
    rows = blocks[0].shape[0] - EXTRA
    before = lax.broadcasted_iota(jnp.int32, (rows, rows), 0)
    after = lax.broadcasted_iota(jnp.int32, (rows, rows), 1)
    upto = (before <= after).astype(jnp.float32).astype(jnp.bfloat16)
    slot = lax.broadcasted_iota(jnp.int32, (slots, rows), 0)
    total = jnp.zeros((2 * slots, own_ref.shape[1]), jnp.float32)
    weights = [
        routing_of(block, jnp.bitwise_xor(member, turn) * rows, live_ref[:1, :], rows)
        for turn, block in enumerate(blocks)
    ]
    counts = [
        jnp.dot(
            (weight > 0.0).astype(jnp.float32).astype(jnp.bfloat16),
            upto,
            preferred_element_type=jnp.float32,
        )
        for weight in weights
    ]
    for turn, block in enumerate(blocks):
        weight, count = weights[turn], counts[turn]
        for before, earlier in enumerate(counts):
            if before != turn:
                ahead = jnp.bitwise_xor(member, before) < jnp.bitwise_xor(member, turn)
                count = count + jnp.where(ahead, earlier[:, rows - 1 :], 0.0)
        place = jnp.where(weight > 0.0, count - 1.0, -1.0).astype(jnp.int32)
        pick = jnp.concatenate(
            [(slot == place[e : e + 1, :]).astype(jnp.float32) for e in range(WAVE)], 0
        ).astype(jnp.bfloat16)
        total = total + jnp.dot(pick, block[:rows, :], preferred_element_type=jnp.float32)
        routing_ref[turn, :WAVE, :] = weight[:WAVE]
        routing_ref[turn, WAVE : 2 * WAVE, :] = place[:WAVE].astype(jnp.float32)
    own_ref[...] = total[:slots].astype(own_ref.dtype)
    other_ref[...] = total[slots:].astype(other_ref.dtype)


def compact_rest_kernel(routing_ref, *refs):
    blocks, (own_ref, other_ref) = refs[:-2], refs[-2:]
    slots = own_ref.shape[0]
    rows = blocks[0].shape[0]
    slot = lax.broadcasted_iota(jnp.int32, (slots, rows), 0)
    total = jnp.zeros((2 * slots, own_ref.shape[1]), jnp.float32)
    for turn, block in enumerate(blocks):
        place = routing_ref[turn, WAVE : 2 * WAVE, :].astype(jnp.int32)
        pick = jnp.concatenate(
            [(slot == place[e : e + 1, :]).astype(jnp.float32) for e in range(WAVE)], 0
        ).astype(jnp.bfloat16)
        total = total + jnp.dot(pick, block[...], preferred_element_type=jnp.float32)
    own_ref[...] = total[:slots].astype(own_ref.dtype)
    other_ref[...] = total[slots:].astype(other_ref.dtype)


def spread_kernel(members, held_ref, came_ref, _, pick_ref, column_ref):
    square, _, core = place_of(members)
    rows = held_ref.shape[2]
    slot = lax.broadcasted_iota(jnp.int32, (CAP, rows), 0)
    for turn in range(members):
        routing = jnp.where(square == core, held_ref[turn], came_ref[turn])
        for e in range(WAVE):
            place = routing[WAVE + e : WAVE + e + 1, :].astype(jnp.int32)
            pick_ref[turn, :, e * CAP : (e + 1) * CAP] = (
                (slot == place).astype(jnp.float32).T.astype(pick_ref.dtype)
            )
        table = jnp.where(slot == 0, routing[0:1, :], jnp.where(slot == 1, routing[1:2, :], 0.0))
        column_ref[turn] = table.T


def with_piece(members, turn, width, held, came, use):
    _, member, core = place_of(members)
    per_half = held[0].shape[1] // width
    block = jnp.bitwise_xor(member, turn)
    columns = pl.ds(pl.multiple_of(block % per_half * width, LANES), width)

    @pl.when(block // per_half == core)
    def _():
        use([half.at[:, columns] for half in held])

    @pl.when(block // per_half != core)
    def _():
        use([half.at[:, columns] for half in came])


def part_kernel(members, own_side, turn, first_ref, rest_ref, *refs):
    held, came, out_ref = refs[:2], refs[2:4], refs[-1]
    first = first_ref.shape[1]
    width = out_ref.shape[1] // 2

    def use(weights):
        for n, weight in enumerate(weights):
            total = sum(
                jnp.dot(rows[...], weight[piece, :], preferred_element_type=jnp.float32)
                for rows, piece in ((first_ref, slice(0, first)), (rest_ref, slice(first, None)))
            )
            out_ref[:, n * width : (n + 1) * width] = total.astype(out_ref.dtype)

    @pl.when(is_side(own_side, members))
    def _():
        with_piece(members, turn, width, held, came, use)


def hidden_kernel(members, own_side, *refs):
    parts, out_ref = refs[:members], refs[-1]
    width = out_ref.shape[1]

    @pl.when(is_side(own_side, members))
    def _():
        gate, up = (
            sum(part[:, n * width : (n + 1) * width].astype(jnp.float32) for part in parts)
            for n in range(2)
        )
        out_ref[...] = (gate / (1.0 + jnp.exp(-gate)) * up).astype(out_ref.dtype)


def down_kernel(members, own_side, turns, *refs):
    count = len(turns)
    hidden, (held, came) = refs[:count], refs[count : count + 2]
    earlier, outs, total_ref = refs[count + 2], refs[count + 3 : -1], refs[-1]
    is_last = earlier.dtype == total_ref.dtype

    def use_turn(rows, is_first):
        def use(weights):
            product = lax.dot_general(
                rows[...],
                weights[0][...],
                (((1,), (1,)), ((), ())),
                preferred_element_type=jnp.float32,
            )
            total_ref[...] = product if is_first else total_ref[...] + product

        return use

    @pl.when(is_side(own_side, members))
    def _():
        if is_last:
            total_ref[...] = earlier[...]
        for n, turn in enumerate(turns):
            use = use_turn(hidden[n], n == 0 and not is_last)
            with_piece(members, turn, hidden[n].shape[1], [held], [came], use)
        first = 0
        for out in outs:
            out[...] = total_ref[:, first : first + out.shape[1]].astype(out.dtype)
            first += out.shape[1]


def expand_kernel(turns, members, held_ref, came_ref, other_ref, pick_ref, column_ref, *outs):
    square, _, core = place_of(members)
    own = jnp.where(square == core, held_ref[...], came_ref[...])
    for turn, out in zip(turns, outs):
        total = None
        for e, slots in enumerate((own, other_ref[...])):
            chosen = jnp.dot(
                pick_ref[turn, :, e * CAP : (e + 1) * CAP],
                slots,
                preferred_element_type=jnp.float32,
            )
            part = column_ref[turn, :, e : e + 1] * chosen
            total = part if total is None else total + part
        out[...] = total.astype(out.dtype)


VMEM = pl.BlockSpec(memory_space=pltpu.VMEM)
SMEM = pl.BlockSpec(memory_space=pltpu.SMEM)
HBM = pl.BlockSpec(memory_space=pltpu.HBM)


def call(kernel, outs, specs, scratch=(), mib=8, space=VMEM, flops=0, aliases={}):
    return pl.pallas_call(
        kernel,
        out_shape=[jax.ShapeDtypeStruct(shape, dtype) for shape, dtype in outs],
        in_specs=specs,
        out_specs=space if isinstance(space, list) else [space] * len(outs),
        scratch_shapes=list(scratch),
        input_output_aliases=aliases,
        compiler_params=pltpu.CompilerParams(vmem_limit_bytes=mib * 1024 * 1024),
        cost_estimate=pl.CostEstimate(flops=flops, bytes_accessed=0, transcendentals=0),
    )


def moved(array, ep_size, tp_size, target):
    targets = {(e, t): target(e, t) for e in range(ep_size) for t in range(tp_size)}
    used = set(targets.values())
    pairs = []
    for (e, t), to in targets.items():
        if to is None:
            (free,) = [core for core in range(tp_size) if (e, core) not in used]
            to = (e, free) if free != t else (e ^ 1, t)
        pairs.append((e * tp_size + t, to[0] * tp_size + to[1]))
    return lax.ppermute(array, ("ep", "tp"), pairs)


def resting(
    tokens, expert_ids, gate_values, group_counts, gate_weight, up_weight, down_weight
):
    ep_size, tp_size = lax.axis_size("ep"), lax.axis_size("tp")
    ep, core = lax.axis_index("ep"), lax.axis_index("tp")
    rows = tokens.shape[0]
    members = TOK_G // rows
    per_core = members // tp_size
    member = ep % members
    thick = gate_weight.shape[0]
    width = tp_size * gate_weight.shape[1] // members
    half_lanes = (thick // LANES + 1) // 2 * LANES
    parts = (half_lanes, thick - half_lanes)
    bf16, f32 = jnp.bfloat16, jnp.float32
    send = functools.partial(moved, ep_size=ep_size, tp_size=tp_size)
    far_first = [members - 1 - n for n in range(members - 1)]

    def crosswise(turn, from_own):
        return lambda e, t: (
            (e ^ turn, tp_size - 1 - t) if (t == e // members) == from_own else None
        )

    def across(from_own):
        return lambda e, t: (
            ((e + members) % ep_size, t) if (t == e // members) == from_own else None
        )

    other_half = [(t, tp_size - 1 - t) for t in range(tp_size)]
    tokens_came = lax.ppermute(tokens, "tp", other_half)
    square = ep // members
    experts = jnp.stack([square, WAVE - 1 - square])[:, None, None]
    named = jnp.where(expert_ids.T[None] == experts, gate_values.T[None], 0.0).sum(1)
    blocks = [((rows + EXTRA, parts[0]), bf16)] * members + [((rows, parts[1]), bf16)] * members
    packed = call(
        functools.partial(pack_held_kernel, members),
        blocks,
        [VMEM, HBM],
        [pltpu.VMEM((EXTRA, parts[0]), bf16), pltpu.SemaphoreType.DMA((members, 3))],
        space=HBM,
    )(named, tokens)
    packed = call(
        functools.partial(pack_came_kernel, members),
        blocks,
        [HBM] * (1 + 2 * members),
        [pltpu.SemaphoreType.DMA((members, 2))],
        space=HBM,
        aliases={1 + n: n for n in range(2 * members)},
    )(tokens_came, *packed)
    arrived = [[packed[0]] + [None] * (members - 1), [packed[members]] + [None] * (members - 1)]
    for part in range(2):
        for turn in far_first:
            arrived[part][turn] = send(packed[part * members + turn], target=crosswise(turn, False))
    weights_came = []
    for weight in (gate_weight, up_weight, down_weight):
        weights_came.append(lax.ppermute(weight, "tp", other_half))
    gate_came, up_came, down_came = weights_came
    up_held, live = call(
        functools.partial(hold_kernel, members),
        [(up_weight.shape, bf16), ((8, rows), jnp.int32)],
        [SMEM, HBM],
        [pltpu.SemaphoreType.DMA],
        space=[HBM, VMEM],
    )(group_counts, up_weight)

    own_first, other_first, routing = call(
        compact_kernel,
        [((CAP, parts[0]), bf16)] * 2 + [((members, 8, rows), f32)],
        [VMEM] * (1 + members),
    )(live, *arrived[0])
    came_first = send(other_first, target=across(True))
    own_rest, other_rest = call(
        compact_rest_kernel, [((CAP, parts[1]), bf16)] * 2, [VMEM] * (1 + members)
    )(routing, *arrived[1])
    came_rest = send(other_rest, target=across(True))

    def sums_of(own_side, slot_rows, after):
        sums, last = {}, list(after)
        for turn in far_first + [0]:
            sums[turn] = call(
                functools.partial(part_kernel, members, own_side, turn),
                [((CAP, 2 * width), bf16)],
                [VMEM] * 6 + [HBM] * len(last),
                mib=16,
                flops=4 * CAP * thick * width,
            )(*slot_rows, gate_weight, up_held, gate_came, up_came, *last)[0]
            last = [sums[turn]]
        came = []
        for turn in far_first + [0]:
            came.append(send(sums[turn], target=crosswise(turn, own_side)))
        return came, sums[0]

    def hidden_of(own_side, sums, after):
        hidden = call(
            functools.partial(hidden_kernel, members, not own_side),
            [((CAP, width), bf16)],
            [VMEM] * members + [HBM],
        )(*sums, after)[0]
        came = {}
        for turn in far_first + [0]:
            came[turn] = send(hidden, target=crosswise(turn, not own_side))
        return came, hidden

    own_sums, own_last = sums_of(True, (own_first, own_rest), [])
    other_sums, other_last = sums_of(False, (came_first, came_rest), [own_last])
    own_hidden, own_last = hidden_of(True, own_sums, other_last)
    other_hidden, other_last = hidden_of(False, other_sums, own_last)

    def down_of(own_side, hidden, after):
        whole, halves = [((CAP, thick), f32)], [((CAP, part), bf16) for part in parts]
        total = [after]
        for turns, outs in (((3, 2), whole), ((1, 0), halves)):
            total = call(
                functools.partial(down_kernel, members, own_side, turns),
                outs,
                [VMEM] * (len(turns) + 3),
                [pltpu.VMEM((CAP, thick), f32)],
                16,
            )(*[hidden[turn] for turn in turns], down_weight, down_came, total[0])
        return total

    other_projected = down_of(False, other_hidden, other_last)
    own_projected = down_of(True, own_hidden, other_projected[0])

    def to_leaver(e, t):
        return ((e + members) % ep_size, e % members // per_core) if t != e // members else None

    came_projected = []
    for part in range(2):
        came_projected.append(send(other_projected[part], target=to_leaver))
    routing_came = lax.ppermute(routing, "tp", other_half)
    projected_came = []
    for part in range(2):
        projected_came.append(lax.ppermute(own_projected[part], "tp", other_half))
    pick, column = call(
        functools.partial(spread_kernel, members),
        [((members, rows, WAVE * CAP), bf16), ((members, rows, LANES), f32)],
        [VMEM] * 2 + [HBM],
    )(routing, routing_came, own_last)

    def rows_of(part, *turns):
        return call(
            functools.partial(expand_kernel, turns, members),
            [((rows, parts[part]), bf16)] * len(turns),
            [VMEM] * 5,
        )(own_projected[part], projected_came[part], came_projected[part], pick, column)

    def back(turn):
        def target(e, t):
            core = e % members // per_core
            return (e ^ turn, core) if (t == core) == (turn > 1) else None

        return target

    here = core == member // per_core
    swap = member % per_core == 1
    low, high = [], []
    for part in range(2):
        near, far = rows_of(part, 1, 3)
        kept, middle = rows_of(part, 0, 2)
        near = lax.ppermute(near, "tp", other_half)
        returned = {}
        for turn, block in ((3, far), (2, middle), (1, near)):
            returned[turn] = send(block, target=back(turn))
        same = jnp.where(here, kept, returned[2])
        other = jnp.where(here, returned[1], returned[3])
        low.append(jnp.where(swap, other, same))
        high.append(jnp.where(swap, same, other))
    return jnp.concatenate(low + high, axis=1)


def shards(tokens, expert_ids, gate_values, group_counts, gate_weight, up_weight, down_weight):
    ep_size, tp_size = lax.axis_size("ep"), lax.axis_size("tp")
    members = TOK_G // tokens.shape[0]
    rests = ep_size == WAVE * members and tp_size == WAVE and members == 2 * tp_size
    return (resting if rests else travelling)(
        tokens, expert_ids, gate_values, group_counts, gate_weight, up_weight, down_weight
    )


def solution(mesh):
    placed = (
        P(("rep", "ep"), "tp"),
        P(("rep", "ep"), None),
        P(("rep", "ep"), None),
        P("rep"),
        P(("rep", "ep"), "tp"),
        P(("rep", "ep"), "tp"),
        P(("rep", "ep"), "tp"),
    )
    return jax.shard_map(
        shards, mesh=mesh, in_specs=placed, out_specs=P(("rep", "ep"), "tp"), check_vma=False
    )
```

```python
import functools

import jax
import jax.numpy as jnp
from jax import lax
from jax.experimental import pallas as pl
from jax.experimental.pallas import tpu as pltpu
from jax.sharding import PartitionSpec as P


D = 3584
FF = 2560
WAVE = 2
MEMBERS = 8
GROUP_EP = 4
TOK_G = 512
CAP = 128
LANES = 128
EXTRA = 8


def as_sent(array):

    def short(part):
        return part.astype(jnp.bfloat16) if part.dtype == jnp.float32 else part

    return jax.tree.map(short, array)


def swapped(array, axis, distance):
    return lax.ppermute(array, axis, [(i, i ^ 1 << distance) for i in range(lax.axis_size(axis))])


def dispatch_slots(expert_ids, gate_values, live_count, expert):
    row_index = jnp.arange(TOK_G, dtype=jnp.int32)
    live_rows = row_index < live_count
    hit_mask = expert_ids == expert
    selected = jnp.logical_and(jnp.any(hit_mask, axis=1), live_rows)
    row_weight = jnp.sum(jnp.where(hit_mask, gate_values, jnp.float32(0.0)), axis=1)
    position = jnp.cumsum(selected.astype(jnp.int32)) - 1
    slot_index = jnp.arange(CAP, dtype=jnp.int32)
    slot_match = jnp.logical_and(position[None, :] == slot_index[:, None], selected[None, :])
    slot_rows = jnp.sum(jnp.where(slot_match, row_index[None, :], 0), axis=1)
    slot_valid = jnp.any(slot_match, axis=1)
    slot_weight = jnp.where(slot_valid, row_weight[slot_rows], jnp.float32(0.0))
    return (slot_rows, slot_weight)


def travelling(tokens, expert_ids, gate_values, group_counts, gate_weight, up_weight, down_weight):
    ep_index = lax.axis_index("ep")
    slice_width = FF // MEMBERS
    group_bits = GROUP_EP.bit_length() - 1
    weight_stack = jnp.stack([gate_weight, up_weight, down_weight])
    rows_held = weight_stack.shape[1]
    pieces = weight_stack.shape[2] // slice_width
    slice_blocks = weight_stack.reshape(3, rows_held, pieces, slice_width).transpose(0, 2, 1, 3)
    fan_out = lax.axis_size("ep") // pieces
    outgoing = jnp.tile(slice_blocks, (1, fan_out, 1, 1))
    arrived = lax.all_to_all(outgoing, "ep", split_axis=1, concat_axis=1, tiled=True)
    columns = arrived.reshape(3, -1, slice_width)
    features = lax.all_gather(tokens, "tp", axis=1, tiled=True)
    group_data = (features, expert_ids, gate_values)
    for bit_level in range(group_bits):
        received = jax.tree.map(
            lambda part, own: part.astype(own.dtype),
            swapped(as_sent(group_data), "ep", bit_level),
            group_data,
        )
        upper_half = ep_index >> bit_level & 1 == 1
        group_data = tuple(
            (
                jnp.where(
                    upper_half, jnp.concatenate([other, own], 0), jnp.concatenate([own, other], 0)
                )
                for own, other in zip(group_data, received)
            )
        )
    group_tokens, group_ids, group_gates = group_data
    live_count = lax.dynamic_index_in_dim(group_counts, ep_index // GROUP_EP, keepdims=False)
    partials = jnp.zeros((group_tokens.shape[0], D), jnp.float32)
    for expert in range(WAVE):
        slot_rows, slot_weight = dispatch_slots(group_ids, group_gates, live_count, expert)
        expert_rows = group_tokens[slot_rows]
        gate_cols = columns[0, expert * D : (expert + 1) * D]
        up_cols = columns[1, expert * D : (expert + 1) * D]
        down_cols = columns[2, expert * D : (expert + 1) * D]
        gate_act = jnp.dot(expert_rows, gate_cols, preferred_element_type=jnp.float32)
        up_act = jnp.dot(expert_rows, up_cols, preferred_element_type=jnp.float32)
        hidden = (jax.nn.silu(gate_act) * up_act).astype(jnp.bfloat16)
        projected = lax.dot_general(
            hidden, down_cols, (((1,), (1,)), ((), ())), preferred_element_type=jnp.float32
        )
        partials = partials.at[slot_rows].add(slot_weight[:, None] * projected)
    rounded = lax.optimization_barrier(partials.astype(jnp.bfloat16)).astype(jnp.float32)
    halved = lax.psum_scatter(
        rounded.astype(jnp.bfloat16), "tp", scatter_dimension=1, tiled=True
    ).astype(jnp.float32)
    for bit_level in reversed(range(group_bits)):
        paired_up = halved.reshape(2, -1, halved.shape[1])
        upper_half = ep_index >> bit_level & 1 == 1
        kept_part = jnp.where(upper_half, paired_up[1], paired_up[0])
        sent_part = jnp.where(upper_half, paired_up[0], paired_up[1])
        halved = kept_part + swapped(sent_part.astype(jnp.bfloat16), "ep", bit_level).astype(
            sent_part.dtype
        )
    return halved.astype(jnp.bfloat16)


def place_of(members):
    ep = lax.axis_index("ep")
    return ep // members, ep % members, lax.axis_index("tp")


def is_side(own_side, members):
    square, _, core = place_of(members)
    return (square == core) == own_side


def piece_copy(half, turn, members, destination, sem):
    _, member, core = place_of(members)
    width = destination.shape[1]
    per_half = half.shape[1] // width
    block = jnp.bitwise_xor(member, turn)
    columns = pl.ds(pl.multiple_of(block % per_half * width, LANES), width)
    return block // per_half == core, pltpu.make_async_copy(half.at[:, columns], destination, sem)


def pack_held_kernel(members, named, held, *refs):
    outs, (table_ref, sem) = refs[:members], refs[members:]
    rows = held.shape[0]
    pieces = [
        piece_copy(held, turn, members, out.at[:rows], sem.at[0, turn])
        for turn, out in enumerate(outs)
    ]
    for is_held, copy in pieces:
        pl.when(is_held)(copy.start)
    rest = named[...]
    table_ref[...] = jnp.zeros(table_ref.shape, table_ref.dtype)
    for term in range(3):
        part = rest.astype(jnp.bfloat16)
        rest = rest - part.astype(jnp.float32)
        table_ref[:WAVE, term * rows : (term + 1) * rows] = part
    tables = [
        pltpu.make_async_copy(table_ref, out.at[rows:], sem.at[1, turn])
        for turn, out in enumerate(outs)
    ]
    for copy in tables:
        copy.start()
    for copy in tables:
        copy.wait()
    for is_held, copy in pieces:
        pl.when(is_held)(copy.wait)


def pack_came_kernel(members, came, *refs):
    outs, sem = refs[members : 2 * members], refs[2 * members]
    rows = came.shape[0]
    pieces = [
        piece_copy(came, turn, members, out.at[:rows], sem.at[turn])
        for turn, out in enumerate(outs)
    ]
    for is_held, copy in pieces:
        pl.when(jnp.logical_not(is_held))(copy.start)
    for is_held, copy in pieces:
        pl.when(jnp.logical_not(is_held))(copy.wait)


def hold_kernel(members, counts, array_ref, out_ref, live_ref, sem):
    copy = pltpu.make_async_copy(array_ref, out_ref, sem)
    copy.start()
    live_ref[...] = jnp.full(live_ref.shape, counts[place_of(members)[0]], live_ref.dtype)
    copy.wait()


def routing_of(block, first, live, rows):
    extra = block[rows:, : 3 * LANES].astype(jnp.float32)
    weight = extra[:, :LANES] + extra[:, LANES : 2 * LANES] + extra[:, 2 * LANES :]
    return jnp.where(lax.broadcasted_iota(jnp.int32, weight.shape, 1) + first < live, weight, 0.0)


def compact_kernel(live_ref, *refs):
    blocks, (own_ref, other_ref, routing_ref) = refs[:-3], refs[-3:]
    member = place_of(len(blocks))[1]
    slots = own_ref.shape[0]
    rows = blocks[0].shape[0] - EXTRA
    before = lax.broadcasted_iota(jnp.int32, (rows, rows), 0)
    after = lax.broadcasted_iota(jnp.int32, (rows, rows), 1)
    upto = (before <= after).astype(jnp.float32).astype(jnp.bfloat16)
    slot = lax.broadcasted_iota(jnp.int32, (slots, rows), 0)
    total = jnp.zeros((2 * slots, own_ref.shape[1]), jnp.float32)
    weights = [
        routing_of(block, jnp.bitwise_xor(member, turn) * rows, live_ref[:1, :], rows)
        for turn, block in enumerate(blocks)
    ]
    counts = [
        jnp.dot(
            (weight > 0.0).astype(jnp.float32).astype(jnp.bfloat16),
            upto,
            preferred_element_type=jnp.float32,
        )
        for weight in weights
    ]
    for turn, block in enumerate(blocks):
        weight, count = weights[turn], counts[turn]
        for before, earlier in enumerate(counts):
            if before != turn:
                ahead = jnp.bitwise_xor(member, before) < jnp.bitwise_xor(member, turn)
                count = count + jnp.where(ahead, earlier[:, rows - 1 :], 0.0)
        place = jnp.where(weight > 0.0, count - 1.0, -1.0).astype(jnp.int32)
        pick = jnp.concatenate(
            [(slot == place[e : e + 1, :]).astype(jnp.float32) for e in range(WAVE)], 0
        ).astype(jnp.bfloat16)
        total = total + jnp.dot(pick, block[:rows, :], preferred_element_type=jnp.float32)
        routing_ref[turn, :WAVE, :] = weight[:WAVE]
        routing_ref[turn, WAVE : 2 * WAVE, :] = place[:WAVE].astype(jnp.float32)
    own_ref[...] = total[:slots].astype(own_ref.dtype)
    other_ref[...] = total[slots:].astype(other_ref.dtype)


def spread_kernel(members, held_ref, came_ref, _, pick_ref, column_ref):
    square, _, core = place_of(members)
    rows = held_ref.shape[2]
    slot = lax.broadcasted_iota(jnp.int32, (CAP, rows), 0)
    for turn in range(members):
        routing = jnp.where(square == core, held_ref[turn], came_ref[turn])
        for e in range(WAVE):
            place = routing[WAVE + e : WAVE + e + 1, :].astype(jnp.int32)
            pick_ref[turn, :, e * CAP : (e + 1) * CAP] = (
                (slot == place).astype(jnp.float32).T.astype(pick_ref.dtype)
            )
        table = jnp.where(slot == 0, routing[0:1, :], jnp.where(slot == 1, routing[1:2, :], 0.0))
        column_ref[turn] = table.T


def with_piece(members, turn, width, held, came, use):
    _, member, core = place_of(members)
    per_half = held[0].shape[1] // width
    block = jnp.bitwise_xor(member, turn)
    columns = pl.ds(pl.multiple_of(block % per_half * width, LANES), width)

    @pl.when(block // per_half == core)
    def _():
        use([half.at[:, columns] for half in held])

    @pl.when(block // per_half != core)
    def _():
        use([half.at[:, columns] for half in came])


def part_kernel(members, own_side, turn, rows_ref, *refs):
    held, came, out_ref = refs[:2], refs[2:4], refs[-1]
    width = out_ref.shape[1] // 2

    def use(weights):
        for n, weight in enumerate(weights):
            out_ref[:, n * width : (n + 1) * width] = jnp.dot(
                rows_ref[...], weight[...], preferred_element_type=jnp.float32
            ).astype(out_ref.dtype)

    @pl.when(is_side(own_side, members))
    def _():
        with_piece(members, turn, width, held, came, use)


def hidden_kernel(members, own_side, *refs):
    parts, out_ref = refs[:members], refs[-1]
    width = out_ref.shape[1]

    @pl.when(is_side(own_side, members))
    def _():
        gate, up = (
            sum(part[:, n * width : (n + 1) * width].astype(jnp.float32) for part in parts)
            for n in range(2)
        )
        out_ref[...] = (gate / (1.0 + jnp.exp(-gate)) * up).astype(out_ref.dtype)


def down_kernel(members, own_side, turns, *refs):
    count = len(turns)
    hidden, (held, came) = refs[:count], refs[count : count + 2]
    earlier, outs, total_ref = refs[count + 2], refs[count + 3 : -1], refs[-1]
    is_last = earlier.dtype == total_ref.dtype

    def use_turn(rows, is_first):
        def use(weights):
            product = lax.dot_general(
                rows[...],
                weights[0][...],
                (((1,), (1,)), ((), ())),
                preferred_element_type=jnp.float32,
            )
            total_ref[...] = product if is_first else total_ref[...] + product

        return use

    @pl.when(is_side(own_side, members))
    def _():
        if is_last:
            total_ref[...] = earlier[...]
        for n, turn in enumerate(turns):
            use = use_turn(hidden[n], n == 0 and not is_last)
            with_piece(members, turn, hidden[n].shape[1], [held], [came], use)
        first = 0
        for out in outs:
            out[...] = total_ref[:, first : first + out.shape[1]].astype(out.dtype)
            first += out.shape[1]


def expand_kernel(turns, members, held_ref, came_ref, other_ref, pick_ref, column_ref, *outs):
    square, _, core = place_of(members)
    own = jnp.where(square == core, held_ref[...], came_ref[...])
    for turn, out in zip(turns, outs):
        total = None
        for e, slots in enumerate((own, other_ref[...])):
            chosen = jnp.dot(
                pick_ref[turn, :, e * CAP : (e + 1) * CAP],
                slots,
                preferred_element_type=jnp.float32,
            )
            part = column_ref[turn, :, e : e + 1] * chosen
            total = part if total is None else total + part
        out[...] = total.astype(out.dtype)


VMEM = pl.BlockSpec(memory_space=pltpu.VMEM)
SMEM = pl.BlockSpec(memory_space=pltpu.SMEM)
HBM = pl.BlockSpec(memory_space=pltpu.HBM)


def call(kernel, outs, specs, scratch=(), mib=8, space=VMEM, flops=0, aliases={}):
    return pl.pallas_call(
        kernel,
        out_shape=[jax.ShapeDtypeStruct(shape, dtype) for shape, dtype in outs],
        in_specs=specs,
        out_specs=space if isinstance(space, list) else [space] * len(outs),
        scratch_shapes=list(scratch),
        input_output_aliases=aliases,
        compiler_params=pltpu.CompilerParams(vmem_limit_bytes=mib * 1024 * 1024),
        cost_estimate=pl.CostEstimate(flops=flops, bytes_accessed=0, transcendentals=0),
    )


def moved(array, ep_size, tp_size, target):
    targets = {(e, t): target(e, t) for e in range(ep_size) for t in range(tp_size)}
    used = set(targets.values())
    pairs = []
    for (e, t), to in targets.items():
        if to is None:
            (free,) = [core for core in range(tp_size) if (e, core) not in used]
            to = (e, free) if free != t else (e ^ 1, t)
        pairs.append((e * tp_size + t, to[0] * tp_size + to[1]))
    return lax.ppermute(array, ("ep", "tp"), pairs)


def resting(
    tokens, expert_ids, gate_values, group_counts, gate_weight, up_weight, down_weight
):
    ep_size, tp_size = lax.axis_size("ep"), lax.axis_size("tp")
    ep, core = lax.axis_index("ep"), lax.axis_index("tp")
    rows = tokens.shape[0]
    members = TOK_G // rows
    per_core = members // tp_size
    member = ep % members
    thick = gate_weight.shape[0]
    width = tp_size * gate_weight.shape[1] // members
    half_lanes = (thick // LANES + 1) // 2 * LANES
    parts = (half_lanes, thick - half_lanes)
    bf16, f32 = jnp.bfloat16, jnp.float32
    send = functools.partial(moved, ep_size=ep_size, tp_size=tp_size)
    far_first = [members - 1 - n for n in range(members - 1)]

    def crosswise(turn, from_own):
        return lambda e, t: (
            (e ^ turn, tp_size - 1 - t) if (t == e // members) == from_own else None
        )

    def across(from_own):
        return lambda e, t: (
            ((e + members) % ep_size, t) if (t == e // members) == from_own else None
        )

    other_half = [(t, tp_size - 1 - t) for t in range(tp_size)]
    tokens_came = lax.ppermute(tokens, "tp", other_half)
    square = ep // members
    experts = jnp.stack([square, WAVE - 1 - square])[:, None, None]
    named = jnp.where(expert_ids.T[None] == experts, gate_values.T[None], 0.0).sum(1)
    blocks = [((rows + EXTRA, thick), bf16)] * members
    packed = call(
        functools.partial(pack_held_kernel, members),
        blocks,
        [VMEM, HBM],
        [pltpu.VMEM((EXTRA, thick), bf16), pltpu.SemaphoreType.DMA((2, members))],
        space=HBM,
    )(named, tokens)
    packed = call(
        functools.partial(pack_came_kernel, members),
        blocks,
        [HBM] * (1 + members),
        [pltpu.SemaphoreType.DMA((members,))],
        space=HBM,
        aliases={1 + turn: turn for turn in range(members)},
    )(tokens_came, *packed)
    arrived = {0: packed[0]}
    for turn in far_first:
        arrived[turn] = send(packed[turn], target=crosswise(turn, False))
    weights_came = []
    for weight in (gate_weight, up_weight, down_weight):
        weights_came.append(lax.ppermute(weight, "tp", other_half))
    gate_came, up_came, down_came = weights_came
    up_held, live = call(
        functools.partial(hold_kernel, members),
        [(up_weight.shape, bf16), ((8, rows), jnp.int32)],
        [SMEM, HBM],
        [pltpu.SemaphoreType.DMA],
        space=[HBM, VMEM],
    )(group_counts, up_weight)

    own_rows, other_rows, routing = call(
        compact_kernel,
        [
            ((CAP, thick), bf16),
            ((CAP, thick), bf16),
            ((members, 8, rows), f32),
        ],
        [VMEM] * (1 + members),
    )(live, *[arrived[turn] for turn in range(members)])
    came_rows = send(other_rows, target=across(True))

    def parts_of(own_side, slot_rows, after):
        parts, last = {}, list(after)
        for turn in far_first + [0]:
            parts[turn] = call(
                functools.partial(part_kernel, members, own_side, turn),
                [((CAP, 2 * width), bf16)],
                [VMEM] * 5 + [HBM] * len(last),
                mib=16,
                flops=4 * CAP * thick * width,
            )(slot_rows, gate_weight, up_held, gate_came, up_came, *last)[0]
            last = [parts[turn]]
        came = []
        for turn in far_first + [0]:
            came.append(send(parts[turn], target=crosswise(turn, own_side)))
        return came, parts[0]

    def hidden_of(own_side, parts, after):
        hidden = call(
            functools.partial(hidden_kernel, members, not own_side),
            [((CAP, width), bf16)],
            [VMEM] * members + [HBM],
        )(*parts, after)[0]
        came = {}
        for turn in far_first + [0]:
            came[turn] = send(hidden, target=crosswise(turn, not own_side))
        return came, hidden

    own_parts, own_last = parts_of(True, own_rows, [])
    other_parts, other_last = parts_of(False, came_rows, [own_last])
    other_hidden, other_last = hidden_of(False, other_parts, other_last)
    own_hidden, own_last = hidden_of(True, own_parts, other_last)

    def down_of(own_side, hidden, after):
        whole, halves = [((CAP, thick), f32)], [((CAP, part), bf16) for part in parts]
        total = [after]
        for turns, outs in (((3, 2), whole), ((1, 0), halves)):
            total = call(
                functools.partial(down_kernel, members, own_side, turns),
                outs,
                [VMEM] * (len(turns) + 3),
                [pltpu.VMEM((CAP, thick), f32)],
                16,
            )(*[hidden[turn] for turn in turns], down_weight, down_came, total[0])
        return total

    other_projected = down_of(False, other_hidden, other_last)
    own_projected = down_of(True, own_hidden, other_projected[0])

    def to_leaver(e, t):
        return ((e + members) % ep_size, e % members // per_core) if t != e // members else None

    came_projected = []
    for part in range(2):
        came_projected.append(send(other_projected[part], target=to_leaver))
    routing_came = lax.ppermute(routing, "tp", other_half)
    projected_came = []
    for part in range(2):
        projected_came.append(lax.ppermute(own_projected[part], "tp", other_half))
    pick, column = call(
        functools.partial(spread_kernel, members),
        [((members, rows, WAVE * CAP), bf16), ((members, rows, LANES), f32)],
        [VMEM] * 2 + [HBM],
    )(routing, routing_came, own_last)

    def rows_of(part, *turns):
        return call(
            functools.partial(expand_kernel, turns, members),
            [((rows, parts[part]), bf16)] * len(turns),
            [VMEM] * 5,
        )(own_projected[part], projected_came[part], came_projected[part], pick, column)

    def back(turn):
        def target(e, t):
            core = e % members // per_core
            return (e ^ turn, core) if (t == core) == (turn > 1) else None

        return target

    here = core == member // per_core
    swap = member % per_core == 1
    low, high = [], []
    for part in range(2):
        near, far = rows_of(part, 1, 3)
        kept, middle = rows_of(part, 0, 2)
        near = lax.ppermute(near, "tp", other_half)
        returned = {}
        for turn, block in ((3, far), (2, middle), (1, near)):
            returned[turn] = send(block, target=back(turn))
        same = jnp.where(here, kept, returned[2])
        other = jnp.where(here, returned[1], returned[3])
        low.append(jnp.where(swap, other, same))
        high.append(jnp.where(swap, same, other))
    return jnp.concatenate(low + high, axis=1)


def shards(tokens, expert_ids, gate_values, group_counts, gate_weight, up_weight, down_weight):
    ep_size, tp_size = lax.axis_size("ep"), lax.axis_size("tp")
    members = TOK_G // tokens.shape[0]
    rests = ep_size == WAVE * members and tp_size == WAVE and members == 2 * tp_size
    return (resting if rests else travelling)(
        tokens, expert_ids, gate_values, group_counts, gate_weight, up_weight, down_weight
    )


def solution(mesh):
    placed = (
        P(("rep", "ep"), "tp"),
        P(("rep", "ep"), None),
        P(("rep", "ep"), None),
        P("rep"),
        P(("rep", "ep"), "tp"),
        P(("rep", "ep"), "tp"),
        P(("rep", "ep"), "tp"),
    )
    return jax.shard_map(
        shards, mesh=mesh, in_specs=placed, out_specs=P(("rep", "ep"), "tp"), check_vma=False
    )
```
